32 devices in a mesh: rep: 2 (over x), dp: 16 (over y, z, core).
Axes of the slice: x: 2, y: 2, z: 4, core: 2. Of those that a mesh axis runs over, the one named last changes fastest.
Arguments:
- x: bfloat16 [32, 2048, 640], P(('rep', 'dp')), parts along dimension 0
- dy: bfloat16 [32, 2048, 640], P(('rep', 'dp')), parts along dimension 0
- w_gate: bfloat16 [2, 640, 2048], replicated
- w_up: bfloat16 [2, 640, 2048], replicated
- w_down: bfloat16 [2, 2048, 640], replicated
- m_w_gate: float32 [2, 640, 2048], P(None, 'dp')
- m_w_up: float32 [2, 640, 2048], P(None, 'dp')
- m_w_down: float32 [2, 2048, 640], P(None, 'dp')
- v_w_gate: float32 [2, 640, 2048], P(None, 'dp')
- v_w_up: float32 [2, 640, 2048], P(None, 'dp')
- v_w_down: float32 [2, 2048, 640], P(None, 'dp')
Outputs:
- output 1: bfloat16 [4, 640, 2048], P('rep'), parts along dimension 0
- output 2: bfloat16 [4, 640, 2048], P('rep'), parts along dimension 0
- output 3: bfloat16 [4, 2048, 640], P('rep'), parts along dimension 0
- output 4: float32 [4, 640, 2048], P('rep', 'dp'), parts along dimension 0
- output 5: float32 [4, 640, 2048], P('rep', 'dp'), parts along dimension 0
- output 6: float32 [4, 2048, 640], P('rep', 'dp'), parts along dimension 0
- output 7: float32 [4, 640, 2048], P('rep', 'dp'), parts along dimension 0
- output 8: float32 [4, 640, 2048], P('rep', 'dp'), parts along dimension 0
- output 9: float32 [4, 2048, 640], P('rep', 'dp'), parts along dimension 0
There are 2 independent parts. The reference program is written for one: setup_inputs(seed, part) draws one part's arguments, and reference() takes and returns one part's arrays. A program takes and returns all parts, laid end to end along the dimension named above; an argument that names none is the same for every part.
All inputs are finite; a program needn't handle non-finite values.
Results may differ from the reference program's by a relative error of at most 0.022.
Values are sent between devices in bfloat16 or wider.
A program may use at most 2 GiB of HBM per device.

```python
import jax
import jax.numpy as jnp
from jax import lax

SEQUENCES = 16
TOKENS = 2048
D = 640
FF = 2048
LAYERS = 2
NAMES = ("w_gate", "w_up", "w_down")
SHAPES = {"w_gate": (LAYERS, D, FF), "w_up": (LAYERS, D, FF), "w_down": (LAYERS, FF, D)}


def bump(key, n, height):
    away = (jnp.arange(n, dtype=jnp.int32) - jax.random.randint(key, (), 0, n, jnp.int32)) % n
    return jnp.where(away < n // 8, height, 1.0)


def together(key, own, strength):
    shared = jax.random.normal(key, own.shape[1:], jnp.float32)
    return (own + strength * shared) * lax.rsqrt(1 + strength * strength)


def setup_inputs(seed: int = 0, part: int = 0) -> dict:
    kx, kdy, ka, kb, kz, kf, kh, kl, *keys = jax.random.split(jax.random.key(seed), 8 + 3 * len(NAMES))
    kx, kdy, ka, kb = (jax.random.fold_in(k, part) for k in (kx, kdy, ka, kb))
    kw, km, kv = (keys[i::3] for i in range(3))
    shape = (SEQUENCES, TOKENS, D)
    much_x, much_dy = jax.random.uniform(kz, (2,), jnp.float32, 0.0, 1.0)
    loud = 2.0 ** jax.random.uniform(jax.random.fold_in(kz, 1), (), jnp.float32, -1.0, 2.0)
    layers = 2.0 ** jax.random.uniform(kl, (LAYERS, 1, 1), jnp.float32, -1.0, 1.0)
    x = together(ka, jax.random.normal(kx, shape, jnp.float32), much_x) * bump(kf, D, 4.0)
    dy = together(kb, jax.random.normal(kdy, shape, jnp.float32), much_dy)
    drawn = {"x": x.astype(jnp.bfloat16), "dy": (loud * dy * (SEQUENCES * TOKENS) ** -0.5).astype(jnp.bfloat16)}
    for key, name in zip(kw, NAMES, strict=True):
        w = jax.random.normal(key, SHAPES[name], jnp.float32) * SHAPES[name][1] ** -0.5
        drawn[name] = (w * {"w_gate": 1.0, "w_up": bump(kh, FF, 4.0), "w_down": layers}[name]).astype(jnp.bfloat16)
    for key, name in zip(km, NAMES, strict=True):
        drawn[f"m_{name}"] = 0.1 * jax.random.normal(key, SHAPES[name], jnp.float32)
    for key, name in zip(kv, NAMES, strict=True):
        drawn[f"v_{name}"] = jax.random.uniform(key, SHAPES[name], jnp.float32, 0.005, 0.015)
    return drawn


def matmul(a, w):
    return jnp.dot(a, w, preferred_element_type=jnp.float32).astype(jnp.bfloat16)


def normed(h):
    wide = h.astype(jnp.float32)
    scale = lax.rsqrt(jnp.mean(wide**2, -1, keepdims=True) + 1e-6)
    return (wide * scale).astype(jnp.bfloat16)


def layer(h, w):
    a = normed(h)
    gate = jnp.dot(a, w["w_gate"], preferred_element_type=jnp.float32)
    up = jnp.dot(a, w["w_up"], preferred_element_type=jnp.float32)
    return h + matmul((jax.nn.silu(gate) * up).astype(jnp.bfloat16), w["w_down"])


def adamw(w, m, v, g):
    m = 0.9 * m + 0.1 * g
    v = 0.95 * v + 0.05 * g * g
    step = m * lax.rsqrt(v + 1e-8) + 0.1 * w
    return (w - 0.02 * step).astype(jnp.bfloat16), m, v


def clipped(gradients, sum_of_squares, count):
    factor = jnp.minimum(1.0, 0.5 * lax.rsqrt(sum_of_squares / count + 1e-30))
    return [g * factor for g in gradients]


def stack(weights, h):
    return lax.scan(lambda h, w: (layer(h, w), None), h, weights)[0]


def reference(x, dy, w_gate, w_up, w_down, m_w_gate, m_w_up, m_w_down, v_w_gate, v_w_up, v_w_down):
    weights = dict(zip(NAMES, (w_gate, w_up, w_down), strict=True))

    def take(so_far, sequence):
        h, by_y = sequence
        _, back = jax.vjp(lambda w: stack(w, h), weights)
        return jax.tree.map(lambda total, term: total + term.astype(jnp.float32), so_far, back(by_y)[0]), None

    none_yet = {name: jnp.zeros(w.shape, jnp.float32) for name, w in weights.items()}
    by_weights, _ = lax.scan(take, none_yet, (x, dy))
    gradients = [by_weights[name].astype(jnp.bfloat16).astype(jnp.float32) for name in NAMES]
    gradients = clipped(gradients, sum(jnp.sum(g * g) for g in gradients), sum(g.size for g in gradients))
    new = [
        adamw(w.astype(jnp.float32), m, v, g)
        for w, m, v, g in zip((w_gate, w_up, w_down), (m_w_gate, m_w_up, m_w_down), (v_w_gate, v_w_up, v_w_down), gradients, strict=True)
    ]
    return tuple(one[which] for which in range(3) for one in new)
```

```python
import jax
import jax.numpy as jnp
from jax import lax
from jax.sharding import PartitionSpec as P

F32, BF16 = jnp.float32, jnp.bfloat16


def dot(a, b, dims):
    return lax.dot_general(a, b, (dims, ((), ())), preferred_element_type=F32)


def normed(h):
    wide = h.astype(F32)
    scale = lax.rsqrt(jnp.mean(wide**2, -1, keepdims=True) + 1e-6)
    return (wide * scale).astype(BF16), scale


def adamw(w, m, v, g):
    m = 0.9 * m + 0.1 * g
    v = 0.95 * v + 0.05 * g * g
    step = m * lax.rsqrt(v + 1e-8) + 0.1 * w
    return (w - 0.02 * step).astype(BF16), m, v


def gated_grads(gate, up, d):
    s = jax.nn.sigmoid(gate)
    silu = gate * s
    return (silu * up).astype(BF16), (d * up * (s + silu * (1 - s))).astype(BF16), (d * silu).astype(BF16)


def solution(mesh):
    n = mesh.shape["dp"]

    def body(x, dy, wg, wu, wd, mg, mu, md, vg, vu, vd):
        x, dy = x[0], dy[0]
        me = lax.axis_index("dp")

        def scatter(g):
            return lax.psum_scatter(g.astype(BF16), "dp", scatter_dimension=0, tiled=True)

        a0, _ = normed(x)
        gate0, up0 = dot(a0, wg[0], ((1,), (0,))), dot(a0, wu[0], ((1,), (0,)))
        inner0 = (jax.nn.silu(gate0) * up0).astype(BF16)
        h1 = x + dot(inner0, wd[0], ((1,), (0,))).astype(BF16)
        a1, s1 = normed(h1)
        gate1, up1 = dot(a1, wg[1], ((1,), (0,))), dot(a1, wu[1], ((1,), (0,)))
        d1 = dot(dy, wd[1], ((1,), (1,))).astype(BF16).astype(F32)
        inner1, dg1, du1 = gated_grads(gate1, up1, d1)
        g_d1 = scatter(dot(inner1, dy, ((0,), (0,))))
        g_g1 = scatter(dot(a1, dg1, ((0,), (0,))))
        g_u1 = scatter(dot(a1, du1, ((0,), (0,))))
        da = (dot(dg1, wg[1], ((1,), (1,))) + dot(du1, wu[1], ((1,), (1,)))).astype(BF16).astype(F32)
        wide = h1.astype(F32)
        dwide = s1 * da - wide * (s1**3 * jnp.mean(da * wide, -1, keepdims=True))
        dh = dy + dwide.astype(BF16)
        g_d0 = scatter(dot(inner0, dh, ((0,), (0,))))
        d0 = dot(dh, wd[0], ((1,), (1,))).astype(BF16).astype(F32)
        _, dg0, du0 = gated_grads(gate0, up0, d0)
        g_g0 = scatter(dot(a0, dg0, ((0,), (0,))))
        g_u0 = scatter(dot(a0, du0, ((0,), (0,))))

        grads = [jnp.stack(p).astype(F32) for p in ((g_g0, g_g1), (g_u0, g_u1), (g_d0, g_d1))]
        count = n * sum(g.size for g in grads)
        squares = lax.psum(sum(jnp.sum(g * g) for g in grads), "dp")
        factor = jnp.minimum(1.0, 0.5 * lax.rsqrt(squares / count + 1e-30))
        new = []
        for w, m, v, g in zip((wg, wu, wd), (mg, mu, md), (vg, vu, vd), grads, strict=True):
            rows = g.shape[1]
            own = lax.dynamic_slice_in_dim(w, me * rows, rows, 1).astype(F32)
            w, m, v = adamw(own, m, v, g * factor)
            new.append((lax.all_gather(w, "dp", axis=1, tiled=True), m, v))
        return tuple(one[which] for which in range(3) for one in new)

    whole, rows = P(), P(None, "dp", None)
    seq, mine = P(("rep", "dp")), P("rep", "dp", None)
    return jax.shard_map(
        body,
        mesh=mesh,
        in_specs=(seq, seq) + (whole,) * 3 + (rows,) * 6,
        out_specs=(P("rep"),) * 3 + (mine,) * 6,
        check_vma=False,
    )
```

```python
import jax
import jax.numpy as jnp
from jax import lax
from jax.experimental import pallas as pl
from jax.experimental.pallas import tpu as pltpu
from jax.sharding import PartitionSpec as P

F32, BF16 = jnp.float32, jnp.bfloat16
MESH = pl.DeviceIdType.MESH
ANY = pl.BlockSpec(memory_space=pl.ANY)
CHIPS = 8
HOPS = CHIPS - 1


def dot(a, b, dims):
    return lax.dot_general(a, b, (dims, ((), ())), preferred_element_type=F32)


def normed(h):
    wide = h.astype(F32)
    scale = lax.rsqrt(jnp.mean(wide**2, -1, keepdims=True) + 1e-6)
    return (wide * scale).astype(BF16), scale


def adamw(w, m, v, g):
    m = 0.9 * m + 0.1 * g
    v = 0.95 * v + 0.05 * g * g
    step = m * lax.rsqrt(v + 1e-8) + 0.1 * w
    return (w - 0.02 * step).astype(BF16), m, v


def gated_grads(gate, up, d):
    s = jax.nn.sigmoid(gate)
    silu = gate * s
    return (silu * up).astype(BF16), (d * up * (s + silu * (1 - s))).astype(BF16), (d * silu).astype(BF16)


class Place:
    def __init__(self):
        self.me = lax.axis_index("dp")
        self.chip, self.core = lax.div(self.me, 2), lax.rem(self.me, 2)
        self.at = self.flip(self.chip)
        self.partner = self.chip * 2 + 1 - self.core

    @staticmethod
    def flip(c):
        half = CHIPS // 2
        return c + lax.div(c, half) * (3 * half - 1 - 2 * c)

    def chip_at(self, offset):
        return self.flip(lax.rem(self.at + offset + 2 * CHIPS, CHIPS))

    def device_at(self, offset):
        return self.chip_at(offset) * 2 + self.core


def remote(src, dst, send, recv, device):
    return pltpu.make_async_remote_copy(src, dst, send, recv, device_id={"dp": device}, device_id_type=MESH)


def greet(n):
    me = lax.axis_index("dp")
    barrier = pltpu.get_barrier_semaphore()

    @pl.loop(1, n)
    def _(j):
        pl.semaphore_signal(barrier, inc=1, device_id={"dp": lax.rem(me + j, n)}, device_id_type=MESH)

    pl.semaphore_wait(barrier, n - 1)


def wide(ref):
    return ref[...].astype(F32)


def comm_kernel(n, count, *refs):
    it = iter(refs)
    take = lambda k: [next(it) for _ in range(k)]
    grads = take(6)
    ws, ms, vs = take(3), take(3), take(3)
    w_out, m_out, v_out = take(3), take(3), take(3)
    own40, peer40, got40, own64, peer64, got64 = take(6)
    w40, w64, m40, m64, v40, v64, squares = take(7)
    local_sem, pair_send, pair_recv, ring_send, ring_recv = take(5)
    sq_send, sq_recv, gat_send, gat_recv, cross_send, cross_recv = take(6)

    here = Place()
    me, core = here.me, here.core
    streams = [(layer, kind) for kind in range(4) for layer in (1, 0)]
    sign = lambda kind: 1 - 2 * (kind % 2)

    def own(layer, kind):
        return (own40 if kind < 2 else own64).at[layer, kind % 2]

    def peer(layer, kind):
        return (peer40 if kind < 2 else peer64).at[layer, kind % 2]

    def got(layer, kind):
        return (got40 if kind < 2 else got64).at[layer, kind % 2]

    def source(layer, kind, of_core):
        g = grads[3 * layer + min(kind, 2)]
        return g.at[:, of_core] if kind < 2 else g.at[:, of_core, kind - 2]

    loads = []

    def load(src, dst):
        c = pltpu.make_async_copy(src, dst, local_sem.at[len(loads)])
        c.start()
        loads.append(c)

    for layer, kind in streams:
        load(source(layer, kind, core), own(layer, kind))
    for side, x40, x64, per in ((ws, w40, w64, True), (ms, m40, m64, False), (vs, v40, v64, False)):
        for i in range(2):
            load(side[i].at[:, me] if per else side[i], x40.at[i])
        load(side[2].at[:, me] if per else side[2], x64)

    greet(n)
    pairs = []
    for i, (layer, kind) in enumerate(streams):
        c = remote(source(layer, kind, 1 - core), peer(layer, kind), pair_send.at[i], pair_recv.at[i], here.partner)
        c.start()
        pairs.append(c)

    def hop(i, layer, kind, t):
        q = here.chip_at(-sign(kind) * (1 + t))
        return remote(own(layer, kind).at[q], got(layer, kind).at[t], ring_send.at[i, t], ring_recv.at[i, t], here.device_at(sign(kind)))

    for i, (layer, kind) in enumerate(streams):
        loads[i].wait()
        pairs[i].wait_recv()
        q = here.chip_at(-sign(kind))
        mine = own(layer, kind).at[q]
        mine[...] = (wide(mine) + wide(peer(layer, kind).at[q])).astype(BF16)
        hop(i, layer, kind, 0).start()

    @pl.loop(1, HOPS)
    def _(t):
        for i, (layer, kind) in enumerate(streams):
            hop(i, layer, kind, t - 1).wait_recv()
            q = here.chip_at(-sign(kind) * (1 + t))
            mine = own(layer, kind).at[q]
            mine[...] = (wide(mine) + wide(peer(layer, kind).at[q]) + wide(got(layer, kind).at[t - 1])).astype(BF16)
            hop(i, layer, kind, t).start()

    total = jnp.zeros((1, 1), F32)
    for i, (layer, kind) in enumerate(streams):
        hop(i, layer, kind, HOPS - 1).wait_recv()
        mine = own(layer, kind).at[here.chip]
        g = (wide(mine) + wide(peer(layer, kind).at[here.chip]) + wide(got(layer, kind).at[HOPS - 1])).astype(BF16)
        mine[...] = g
        g = g.astype(F32)
        total += jnp.sum(g * g, keepdims=True)

    squares[me] = jnp.broadcast_to(total, squares.shape[1:])

    def tell(j):
        return remote(squares.at[me], squares.at[me], sq_send.at[j], sq_recv.at[me], lax.rem(me + j, n))

    def told(j):
        o = lax.rem(me + n - j, n)
        return remote(squares.at[o], squares.at[o], sq_send.at[j], sq_recv.at[o], o)

    @pl.loop(1, n)
    def _(j):
        tell(j).start()

    for c in loads[len(streams) :]:
        c.wait()

    @pl.loop(1, n)
    def _(j):
        told(j).wait_recv()

    total = jnp.sum(squares[...], axis=0)[:1, :1]
    factor = jnp.minimum(1.0, 0.5 * lax.rsqrt(total / count + 1e-30))

    def whole(layer, kind, owner):
        return w_out[kind].at[layer, owner] if kind < 2 else w_out[2].at[layer, owner, kind - 2]

    def pass_on(i, layer, kind, t):
        o = here.device_at(-sign(kind) * t)
        block = whole(layer, kind, o)
        return remote(block, block, gat_send.at[i, t], gat_recv.at[i, t], here.device_at(sign(kind)))

    def across(i, layer, kind, t):
        o = here.device_at(-sign(kind) * t)
        block = whole(layer, kind, o)
        return remote(block, block, cross_send.at[i, t], cross_recv.at[i, t], here.partner)

    def across_in(i, layer, kind, t):
        o = here.chip_at(-sign(kind) * t) * 2 + 1 - core
        block = whole(layer, kind, o)
        return remote(block, block, cross_send.at[i, t], cross_recv.at[i, t], here.partner)

    for i, (layer, kind) in enumerate(streams):
        sel = (lambda r40, r64: r40.at[kind, layer] if kind < 2 else r64.at[layer, kind - 2])
        out = (lambda r: r[kind].at[layer] if kind < 2 else r[2].at[layer, kind - 2])
        g = wide(own(layer, kind).at[here.chip]) * factor
        w, m, v = adamw(wide(sel(w40, w64)), sel(m40, m64)[...], sel(v40, v64)[...], g)
        whole(layer, kind, me)[...] = w
        pass_on(i, layer, kind, 0).start()
        across(i, layer, kind, 0).start()
        out(m_out)[...] = m
        out(v_out)[...] = v

    @pl.loop(1, HOPS)
    def _(t):
        for i, (layer, kind) in enumerate(streams):
            pass_on(i, layer, kind, t - 1).wait_recv()
            pass_on(i, layer, kind, t).start()
            across(i, layer, kind, t).start()

    for i, (layer, kind) in enumerate(streams):
        pass_on(i, layer, kind, HOPS - 1).wait_recv()
        across(i, layer, kind, HOPS).start()

    for i, (layer, kind) in enumerate(streams):
        pairs[i].wait_send()

    @pl.loop(0, HOPS)
    def _(t):
        for i, (layer, kind) in enumerate(streams):
            hop(i, layer, kind, t).wait_send()
            pass_on(i, layer, kind, t).wait_send()

    @pl.loop(1, n)
    def _(j):
        tell(j).wait_send()

    @pl.loop(0, CHIPS)
    def _(t):
        for i, (layer, kind) in enumerate(streams):
            across(i, layer, kind, t).wait_send()
            across_in(i, layer, kind, t).wait_recv()


def comm(n, count, grads, ws, ms, vs):
    dma = pltpu.SemaphoreType.DMA
    two = lambda k: [pltpu.VMEM((2, 2, k, 40, 2048), BF16), pltpu.VMEM((2, 2, k, 64, 640), BF16)]
    own, peer, got = two(CHIPS), two(CHIPS), two(HOPS)
    scratch = [own[0], peer[0], got[0], own[1], peer[1], got[1]]
    scratch += [pltpu.VMEM((2, 2, 40, 2048), BF16), pltpu.VMEM((2, 2, 64, 640), BF16)]
    scratch += [pltpu.VMEM((2, 2, 40, 2048), F32), pltpu.VMEM((2, 2, 64, 640), F32)] * 2
    scratch += [pltpu.VMEM((n, 8, 128), F32)]
    scratch += [dma((17,)), dma((8,)), dma((8,)), dma((8, HOPS)), dma((8, HOPS)), dma((n,)), dma((n,))]
    scratch += [dma((8, HOPS)), dma((8, HOPS)), dma((8, CHIPS)), dma((8, CHIPS))]
    out_shape = [pltpu.VMEM((2, n, 40, 2048), BF16)] * 2 + [pltpu.VMEM((2, n, 2, 64, 640), BF16)]
    out_shape += ([pltpu.VMEM((2, 40, 2048), F32)] * 2 + [pltpu.VMEM((2, 2, 64, 640), F32)]) * 2
    return pl.pallas_call(
        lambda *refs: comm_kernel(n, count, *refs),
        out_shape=out_shape,
        in_specs=[ANY] * 15,
        out_specs=[pl.BlockSpec(memory_space=pltpu.VMEM)] * 9,
        scratch_shapes=scratch,
        compiler_params=pltpu.CompilerParams(collective_id=0, has_side_effects=True, vmem_limit_bytes=40 * 2**20),
        name="comm",
    )(*grads, *ws, *ms, *vs)


def write_kernel(*refs):
    k = (len(refs) - 1) // 2
    copies = [pltpu.make_async_copy(refs[i], refs[k + i], refs[-1].at[i]) for i in range(k)]
    for c in copies:
        c.start()
    for c in copies:
        c.wait()


def write(arrays):
    return pl.pallas_call(
        write_kernel,
        out_shape=[jax.ShapeDtypeStruct(a.shape, a.dtype) for a in arrays],
        in_specs=[pl.BlockSpec(memory_space=pltpu.VMEM)] * len(arrays),
        out_specs=[ANY] * len(arrays),
        scratch_shapes=[pltpu.SemaphoreType.DMA((len(arrays),))],
        compiler_params=pltpu.CompilerParams(vmem_limit_bytes=2**20),
        name="write",
    )(*arrays)


def solution(mesh):
    n = mesh.shape["dp"]

    def body(x, dy, wg, wu, wd, mg, mu, md, vg, vu, vd):
        x, dy = x[0], dy[0]
        a0, _ = normed(x)
        gate0, up0 = dot(a0, wg[0], ((1,), (0,))), dot(a0, wu[0], ((1,), (0,)))
        inner0 = (jax.nn.silu(gate0) * up0).astype(BF16)
        h1 = x + dot(inner0, wd[0], ((1,), (0,))).astype(BF16)
        a1, s1 = normed(h1)
        gate1, up1 = dot(a1, wg[1], ((1,), (0,))), dot(a1, wu[1], ((1,), (0,)))
        d1 = dot(dy, wd[1], ((1,), (1,))).astype(BF16).astype(F32)
        inner1, dg1, du1 = gated_grads(gate1, up1, d1)
        g_d1 = dot(inner1, dy, ((0,), (0,))).astype(BF16)
        g_g1 = dot(a1, dg1, ((0,), (0,))).astype(BF16)
        g_u1 = dot(a1, du1, ((0,), (0,))).astype(BF16)
        da = (dot(dg1, wg[1], ((1,), (1,))) + dot(du1, wu[1], ((1,), (1,)))).astype(BF16).astype(F32)
        h = h1.astype(F32)
        dh = dy + (s1 * da - h * (s1**3 * jnp.mean(da * h, -1, keepdims=True))).astype(BF16)
        g_d0 = dot(inner0, dh, ((0,), (0,))).astype(BF16)
        d0 = dot(dh, wd[0], ((1,), (1,))).astype(BF16).astype(F32)
        _, dg0, du0 = gated_grads(gate0, up0, d0)
        g_g0 = dot(a0, dg0, ((0,), (0,))).astype(BF16)
        g_u0 = dot(a0, du0, ((0,), (0,))).astype(BF16)

        flat = lambda g: g.reshape(CHIPS, 2, 40, 2048)
        grads = [flat(g_g0), flat(g_u0), g_d0.reshape(CHIPS, 2, 2, 64, 640)]
        grads += [flat(g_g1), flat(g_u1), g_d1.reshape(CHIPS, 2, 2, 64, 640)]
        rows = lambda w: w.reshape(2, n, 40, 2048)
        ws = [rows(wg), rows(wu), wd.reshape(2, n, 2, 64, 640)]
        split = lambda t: t.reshape(2, 2, 64, 640)
        count = wg.size + wu.size + wd.size
        outs = write(comm(n, count, grads, ws, [mg, mu, split(md)], [vg, vu, split(vd)]))
        shapes = [wg, wu, wd, mg, mu, md, vg, vu, vd]
        return tuple(o.reshape(s.shape) for o, s in zip(outs, shapes, strict=True))

    whole, mine = P(), P(None, "dp", None)
    seq, out = P(("rep", "dp")), P("rep", "dp", None)
    return jax.shard_map(
        body,
        mesh=mesh,
        in_specs=(seq, seq) + (whole,) * 3 + (mine,) * 6,
        out_specs=(P("rep"),) * 3 + (out,) * 6,
        check_vma=False,
    )
```

```python
import jax
import jax.numpy as jnp
from jax import lax
from jax.experimental import pallas as pl
from jax.experimental.pallas import tpu as pltpu
from jax.sharding import PartitionSpec as P

F32, BF16 = jnp.float32, jnp.bfloat16
MESH = pl.DeviceIdType.MESH
ANY = pl.BlockSpec(memory_space=pl.ANY)
CHIPS = 8
HOPS = CHIPS - 1


def dot(a, b, dims):
    return lax.dot_general(a, b, (dims, ((), ())), preferred_element_type=F32)


def normed(h):
    wide = h.astype(F32)
    scale = lax.rsqrt(jnp.mean(wide**2, -1, keepdims=True) + 1e-6)
    return (wide * scale).astype(BF16), scale


def adamw(w, m, v, g):
    m = 0.9 * m + 0.1 * g
    v = 0.95 * v + 0.05 * g * g
    step = m * lax.rsqrt(v + 1e-8) + 0.1 * w
    return (w - 0.02 * step).astype(BF16), m, v


TILE = 512
FB = 256


def tiles(tokens):
    return [pl.ds(r, TILE) for r in range(0, tokens, TILE)]


def nn(a, b):
    return dot(a, b, ((1,), (0,)))


def nt(a, b):
    return dot(a, b, ((1,), (1,)))


def gates(a, wg, wu):
    gate, up = nn(a, wg), nn(a, wu)
    s = 0.5 + 0.5 * jnp.tanh(0.5 * gate)
    silu = gate * s
    return silu, up * (s + silu * (1 - s)), (silu * up).astype(BF16)


def forward_kernel(x, dy, wg, wu, wd, silu_out, slope_out, inner_out, at_out, dyt_out, h_out, a_out, a, acc):
    j = pl.program_id(0)
    tokens = x.shape[0]

    @pl.when(j == 0)
    def _():
        for r in tiles(tokens):
            a[r] = normed(x[r])[0]
            acc[r] = jnp.zeros((TILE, x.shape[1]), F32)

    part = pl.ds(pl.multiple_of(j * FB, FB), FB)
    at_out[...] = a[part].T
    dyt_out[...] = dy[part].T
    for r in tiles(tokens):
        silu, slope, inner = gates(a[r], wg[...], wu[...])
        silu_out[r], slope_out[r], inner_out[r] = silu, slope, inner
        acc[r] += nn(inner, wd[...])

    @pl.when(j == pl.num_programs(0) - 1)
    def _():
        for r in tiles(tokens):
            h = x[r] + acc[r].astype(BF16)
            h_out[r] = h
            a_out[r] = normed(h)[0]


def forward(x, dy, wg, wu, wd):
    tokens, d = x.shape
    steps = tokens // FB
    whole = lambda s: pl.BlockSpec(s, lambda j: (0, 0))
    cols = lambda rows: pl.BlockSpec((rows, FB), lambda j: (0, j))
    wcols = pl.BlockSpec((None, d, FB), lambda j: (0, 0, j))
    wrows = pl.BlockSpec((None, FB, d), lambda j: (0, j, 0))
    ff = wg.shape[2]
    shape = jax.ShapeDtypeStruct
    return pl.pallas_call(
        forward_kernel,
        grid=(ff // FB,),
        in_specs=[whole(x.shape), whole(x.shape), wcols, wcols, wrows],
        out_specs=[cols(tokens), cols(tokens), cols(tokens), cols(d), cols(d), whole(x.shape), whole(x.shape)],
        out_shape=[shape((tokens, ff), F32)] * 2
        + [shape((tokens, ff), BF16)]
        + [shape((d, tokens), BF16)] * 2
        + [shape(x.shape, BF16)] * 2,
        scratch_shapes=[pltpu.VMEM(x.shape, BF16), pltpu.VMEM(x.shape, F32)],
        compiler_params=pltpu.CompilerParams(vmem_limit_bytes=60 * 2**20),
        name="forward",
    )(x, dy, wg, wu, wd)


def store_gradients(outs, dyt, at, inner, dg, du):
    gate_out, up_out, down_out = outs
    down_out[...] = nn(dyt[...], inner[...]).T.reshape(down_out.shape).astype(BF16)
    gate_out[...] = nn(at[...], dg[...]).reshape(gate_out.shape).astype(BF16)
    up_out[...] = nn(at[...], du[...]).reshape(up_out.shape).astype(BF16)


def backward_kernel(dy_in, a_in, h_in, dyt_in, a0t_in, wg, wu, wd, silu, slope, inner0, *refs):
    outs1, outs0 = refs[0:3], refs[3:6]
    d, a, h, dt, at, da, inner, dg, du, sems = refs[6:]
    step = pl.program_id(0)
    half = pl.num_programs(0) // 2
    tokens = d.shape[0]

    def load(src, dst, i):
        return pltpu.make_async_copy(src, dst, sems.at[i])

    @pl.when(step == 0)
    def _():
        first = [load(dy_in, d, 0), load(a_in, a, 1), load(dyt_in, dt, 2), load(h_in, h, 3)]
        for c in first:
            c.start()
        for r in tiles(tokens):
            da[r] = jnp.zeros((TILE, d.shape[1]), F32)
        for c in first:
            c.wait()
        at[...] = a[...].T

    @pl.when(step < half)
    def _():
        both = jnp.concatenate([wg[...], wu[...]], axis=1)
        for r in tiles(tokens):
            by_inner = nt(d[r], wd[...]).astype(BF16).astype(F32)
            silu, slope, product = gates(a[r], wg[...], wu[...])
            by_gate, by_up = (by_inner * slope).astype(BF16), (by_inner * silu).astype(BF16)
            inner[r], dg[r], du[r] = product, by_gate, by_up
            da[r] += nt(jnp.concatenate([by_gate, by_up], axis=1), both)
        store_gradients(outs1, dt, at, inner, dg, du)

    @pl.when(step == half - 1)
    def _():
        c = load(a0t_in, at, 0)
        c.start()
        for r in tiles(tokens):
            wide = h[r].astype(F32)
            scale = lax.rsqrt(jnp.mean(wide**2, -1, keepdims=True) + 1e-6)
            by_a = da[r].astype(BF16).astype(F32)
            by_h = scale * by_a - wide * (scale**3 * jnp.mean(by_a * wide, -1, keepdims=True))
            d[r] = d[r] + by_h.astype(BF16)
        dt[...] = d[...].T
        c.wait()

    @pl.when(step >= half)
    def _():
        for r in tiles(tokens):
            by_inner = nt(d[r], wd[...]).astype(BF16).astype(F32)
            dg[r], du[r] = (by_inner * slope[r]).astype(BF16), (by_inner * silu[r]).astype(BF16)
        store_gradients(outs0, dt, at, inner0, dg, du)


def backward(n, dy, a1, h1, dyt, a0t, wg, wu, wd, silu, slope, inner0):
    tokens, d = dy.shape
    ff = wg.shape[2]
    half = ff // FB
    early = lambda s: jnp.minimum(s, half - 1)
    late = lambda s: jnp.maximum(s - half, 0)
    layer = lambda s: 1 - s // half
    wcols = pl.BlockSpec((None, d, FB), lambda s: (1, 0, early(s)))
    wrows = pl.BlockSpec((None, FB, d), lambda s: (layer(s), s % half, 0))
    saved = pl.BlockSpec((tokens, FB), lambda s: (0, late(s)))

    def outs(at):
        cols = pl.BlockSpec((n, d // n, FB), lambda s: (0, 0, at(s)))
        return [cols, cols, pl.BlockSpec((FB * n // ff, 2, ff // n // 2, d), lambda s: (at(s), 0, 0, 0))]

    shape = lambda *s: jax.ShapeDtypeStruct(s, BF16)
    shapes = [shape(n, d // n, ff)] * 2 + [shape(n, 2, ff // n // 2, d)]
    rows, block = pltpu.VMEM((tokens, d), BF16), pltpu.VMEM((tokens, FB), BF16)
    flipped = pltpu.VMEM((d, tokens), BF16)
    return pl.pallas_call(
        backward_kernel,
        grid=(2 * half,),
        in_specs=[ANY] * 5 + [wcols, wcols, wrows, saved, saved, saved],
        out_specs=outs(early) + outs(late),
        out_shape=shapes * 2,
        scratch_shapes=[rows, rows, rows, flipped, flipped, pltpu.VMEM((tokens, d), F32), block, block, block]
        + [pltpu.SemaphoreType.DMA((4,))],
        compiler_params=pltpu.CompilerParams(vmem_limit_bytes=60 * 2**20),
        name="backward",
    )(dy, a1, h1, dyt, a0t, wg, wu, wd, silu, slope, inner0)


class Place:
    def __init__(self):
        self.me = lax.axis_index("dp")
        self.chip, self.core = lax.div(self.me, 2), lax.rem(self.me, 2)
        self.at = self.flip(self.chip)
        self.partner = self.chip * 2 + 1 - self.core

    @staticmethod
    def flip(c):
        half = CHIPS // 2
        return c + lax.div(c, half) * (3 * half - 1 - 2 * c)

    def chip_at(self, offset):
        return self.flip(lax.rem(self.at + offset + 2 * CHIPS, CHIPS))

    def device_at(self, offset):
        return self.chip_at(offset) * 2 + self.core


def remote(src, dst, send, recv, device):
    return pltpu.make_async_remote_copy(src, dst, send, recv, device_id={"dp": device}, device_id_type=MESH)


def greet(n):
    me = lax.axis_index("dp")
    barrier = pltpu.get_barrier_semaphore()

    @pl.loop(1, n)
    def _(j):
        pl.semaphore_signal(barrier, inc=1, device_id={"dp": lax.rem(me + j, n)}, device_id_type=MESH)

    pl.semaphore_wait(barrier, n - 1)


def wide(ref):
    return ref[...].astype(F32)


def comm_kernel(n, count, *refs):
    it = iter(refs)
    take = lambda k: [next(it) for _ in range(k)]
    grads = take(6)
    ws, ms, vs = take(3), take(3), take(3)
    w_out, m_out, v_out = take(3), take(3), take(3)
    own40, peer40, got40, own64, peer64, got64 = take(6)
    w40, w64, m40, m64, v40, v64, squares = take(7)
    local_sem, pair_send, pair_recv, ring_send, ring_recv = take(5)
    sq_send, sq_recv, gat_send, gat_recv, cross_send, cross_recv = take(6)

    here = Place()
    me, core = here.me, here.core
    streams = [(layer, kind) for kind in range(4) for layer in (1, 0)]
    sign = lambda kind: 1 - 2 * (kind % 2)

    def own(layer, kind):
        return (own40 if kind < 2 else own64).at[layer, kind % 2]

    def peer(layer, kind):
        return (peer40 if kind < 2 else peer64).at[layer, kind % 2]

    def got(layer, kind):
        return (got40 if kind < 2 else got64).at[layer, kind % 2]

    def source(layer, kind, of_core):
        g = grads[3 * layer + min(kind, 2)]
        return g.at[:, of_core] if kind < 2 else g.at[:, of_core, kind - 2]

    loads = []

    def load(src, dst):
        c = pltpu.make_async_copy(src, dst, local_sem.at[len(loads)])
        c.start()
        loads.append(c)

    for layer, kind in streams:
        load(source(layer, kind, core), own(layer, kind))
    for side, x40, x64, per in ((ws, w40, w64, True), (ms, m40, m64, False), (vs, v40, v64, False)):
        for i in range(2):
            load(side[i].at[:, me] if per else side[i], x40.at[i])
        load(side[2].at[:, me] if per else side[2], x64)

    greet(n)
    pairs = []
    for i, (layer, kind) in enumerate(streams):
        c = remote(source(layer, kind, 1 - core), peer(layer, kind), pair_send.at[i], pair_recv.at[i], here.partner)
        c.start()
        pairs.append(c)

    def hop(i, layer, kind, t):
        q = here.chip_at(-sign(kind) * (1 + t))
        return remote(own(layer, kind).at[q], got(layer, kind).at[t], ring_send.at[i, t], ring_recv.at[i, t], here.device_at(sign(kind)))

    for i, (layer, kind) in enumerate(streams):
        loads[i].wait()
        pairs[i].wait_recv()
        q = here.chip_at(-sign(kind))
        mine = own(layer, kind).at[q]
        mine[...] = (wide(mine) + wide(peer(layer, kind).at[q])).astype(BF16)
        hop(i, layer, kind, 0).start()

    @pl.loop(1, HOPS)
    def _(t):
        for i, (layer, kind) in enumerate(streams):
            hop(i, layer, kind, t - 1).wait_recv()
            q = here.chip_at(-sign(kind) * (1 + t))
            mine = own(layer, kind).at[q]
            mine[...] = (wide(mine) + wide(peer(layer, kind).at[q]) + wide(got(layer, kind).at[t - 1])).astype(BF16)
            hop(i, layer, kind, t).start()

    total = jnp.zeros((1, 1), F32)
    for i, (layer, kind) in enumerate(streams):
        hop(i, layer, kind, HOPS - 1).wait_recv()
        mine = own(layer, kind).at[here.chip]
        g = (wide(mine) + wide(peer(layer, kind).at[here.chip]) + wide(got(layer, kind).at[HOPS - 1])).astype(BF16)
        mine[...] = g
        g = g.astype(F32)
        total += jnp.sum(g * g, keepdims=True)

    squares[me] = jnp.broadcast_to(total, squares.shape[1:])

    def tell(j):
        return remote(squares.at[me], squares.at[me], sq_send.at[j], sq_recv.at[me], lax.rem(me + j, n))

    def told(j):
        o = lax.rem(me + n - j, n)
        return remote(squares.at[o], squares.at[o], sq_send.at[j], sq_recv.at[o], o)

    @pl.loop(1, n)
    def _(j):
        tell(j).start()

    for c in loads[len(streams) :]:
        c.wait()

    @pl.loop(1, n)
    def _(j):
        told(j).wait_recv()

    total = jnp.sum(squares[...], axis=0)[:1, :1]
    factor = jnp.minimum(1.0, 0.5 * lax.rsqrt(total / count + 1e-30))

    def whole(layer, kind, owner):
        return w_out[kind].at[layer, owner] if kind < 2 else w_out[2].at[layer, owner, kind - 2]

    def pass_on(i, layer, kind, t):
        o = here.device_at(-sign(kind) * t)
        block = whole(layer, kind, o)
        return remote(block, block, gat_send.at[i, t], gat_recv.at[i, t], here.device_at(sign(kind)))

    def across(i, layer, kind, t):
        o = here.device_at(-sign(kind) * t)
        block = whole(layer, kind, o)
        return remote(block, block, cross_send.at[i, t], cross_recv.at[i, t], here.partner)

    def across_in(i, layer, kind, t):
        o = here.chip_at(-sign(kind) * t) * 2 + 1 - core
        block = whole(layer, kind, o)
        return remote(block, block, cross_send.at[i, t], cross_recv.at[i, t], here.partner)

    for i, (layer, kind) in enumerate(streams):
        sel = (lambda r40, r64: r40.at[kind, layer] if kind < 2 else r64.at[layer, kind - 2])
        out = (lambda r: r[kind].at[layer] if kind < 2 else r[2].at[layer, kind - 2])
        g = wide(own(layer, kind).at[here.chip]) * factor
        w, m, v = adamw(wide(sel(w40, w64)), sel(m40, m64)[...], sel(v40, v64)[...], g)
        whole(layer, kind, me)[...] = w
        pass_on(i, layer, kind, 0).start()
        across(i, layer, kind, 0).start()
        out(m_out)[...] = m
        out(v_out)[...] = v

    @pl.loop(1, HOPS)
    def _(t):
        for i, (layer, kind) in enumerate(streams):
            pass_on(i, layer, kind, t - 1).wait_recv()
            pass_on(i, layer, kind, t).start()
            across(i, layer, kind, t).start()

    for i, (layer, kind) in enumerate(streams):
        pass_on(i, layer, kind, HOPS - 1).wait_recv()
        across(i, layer, kind, HOPS).start()

    for i, (layer, kind) in enumerate(streams):
        pairs[i].wait_send()

    @pl.loop(0, HOPS)
    def _(t):
        for i, (layer, kind) in enumerate(streams):
            hop(i, layer, kind, t).wait_send()
            pass_on(i, layer, kind, t).wait_send()

    @pl.loop(1, n)
    def _(j):
        tell(j).wait_send()

    @pl.loop(0, CHIPS)
    def _(t):
        for i, (layer, kind) in enumerate(streams):
            across(i, layer, kind, t).wait_send()
            across_in(i, layer, kind, t).wait_recv()


def comm(n, count, grads, ws, ms, vs):
    dma = pltpu.SemaphoreType.DMA
    two = lambda k: [pltpu.VMEM((2, 2, k, 40, 2048), BF16), pltpu.VMEM((2, 2, k, 64, 640), BF16)]
    own, peer, got = two(CHIPS), two(CHIPS), two(HOPS)
    scratch = [own[0], peer[0], got[0], own[1], peer[1], got[1]]
    scratch += [pltpu.VMEM((2, 2, 40, 2048), BF16), pltpu.VMEM((2, 2, 64, 640), BF16)]
    scratch += [pltpu.VMEM((2, 2, 40, 2048), F32), pltpu.VMEM((2, 2, 64, 640), F32)] * 2
    scratch += [pltpu.VMEM((n, 8, 128), F32)]
    scratch += [dma((17,)), dma((8,)), dma((8,)), dma((8, HOPS)), dma((8, HOPS)), dma((n,)), dma((n,))]
    scratch += [dma((8, HOPS)), dma((8, HOPS)), dma((8, CHIPS)), dma((8, CHIPS))]
    out_shape = [pltpu.VMEM((2, n, 40, 2048), BF16)] * 2 + [pltpu.VMEM((2, n, 2, 64, 640), BF16)]
    out_shape += ([pltpu.VMEM((2, 40, 2048), F32)] * 2 + [pltpu.VMEM((2, 2, 64, 640), F32)]) * 2
    return pl.pallas_call(
        lambda *refs: comm_kernel(n, count, *refs),
        out_shape=out_shape,
        in_specs=[ANY] * 15,
        out_specs=[pl.BlockSpec(memory_space=pltpu.VMEM)] * 9,
        scratch_shapes=scratch,
        compiler_params=pltpu.CompilerParams(collective_id=0, has_side_effects=True, vmem_limit_bytes=40 * 2**20),
        name="comm",
    )(*grads, *ws, *ms, *vs)


def write_kernel(*refs):
    k = (len(refs) - 1) // 2
    copies = [pltpu.make_async_copy(refs[i], refs[k + i], refs[-1].at[i]) for i in range(k)]
    for c in copies:
        c.start()
    for c in copies:
        c.wait()


def write(arrays):
    return pl.pallas_call(
        write_kernel,
        out_shape=[jax.ShapeDtypeStruct(a.shape, a.dtype) for a in arrays],
        in_specs=[pl.BlockSpec(memory_space=pltpu.VMEM)] * len(arrays),
        out_specs=[ANY] * len(arrays),
        scratch_shapes=[pltpu.SemaphoreType.DMA((len(arrays),))],
        compiler_params=pltpu.CompilerParams(vmem_limit_bytes=2**20),
        name="write",
    )(*arrays)


def solution(mesh):
    n = mesh.shape["dp"]

    def body(x, dy, wg, wu, wd, mg, mu, md, vg, vu, vd):
        x, dy = x[0], dy[0]
        silu, slope, inner0, a0t, dyt, h1, a1 = forward(x, dy, wg, wu, wd)
        grads = backward(n, dy, a1, h1, dyt, a0t, wg, wu, wd, silu, slope, inner0)
        by = lambda g: g.reshape(CHIPS, 2, *g.shape[1:])
        grads = [by(g) for g in grads[3:] + grads[:3]]
        rows = lambda w: w.reshape(2, n, 40, 2048)
        ws = [rows(wg), rows(wu), wd.reshape(2, n, 2, 64, 640)]
        split = lambda t: t.reshape(2, 2, 64, 640)
        count = wg.size + wu.size + wd.size
        outs = write(comm(n, count, grads, ws, [mg, mu, split(md)], [vg, vu, split(vd)]))
        shapes = [wg, wu, wd, mg, mu, md, vg, vu, vd]
        return tuple(o.reshape(s.shape) for o, s in zip(outs, shapes, strict=True))

    whole, mine = P(), P(None, "dp", None)
    seq, out = P(("rep", "dp")), P("rep", "dp", None)
    return jax.shard_map(
        body,
        mesh=mesh,
        in_specs=(seq, seq) + (whole,) * 3 + (mine,) * 6,
        out_specs=(P("rep"),) * 3 + (out,) * 6,
        check_vma=False,
    )
```

```python
import jax
import jax.numpy as jnp
from jax import lax
from jax.experimental import pallas as pl
from jax.experimental.pallas import tpu as pltpu
from jax.sharding import PartitionSpec as P

F32, BF16 = jnp.float32, jnp.bfloat16
MESH = pl.DeviceIdType.MESH
ANY = pl.BlockSpec(memory_space=pl.ANY)
CHIPS = 8
HOPS = CHIPS - 1


def dot(a, b, dims):
    return lax.dot_general(a, b, (dims, ((), ())), preferred_element_type=F32)


def normed(h):
    wide = h.astype(F32)
    scale = lax.rsqrt(jnp.mean(wide**2, -1, keepdims=True) + 1e-6)
    return (wide * scale).astype(BF16), scale


def adamw(w, m, v, g):
    m = 0.9 * m + 0.1 * g
    v = 0.95 * v + 0.05 * g * g
    step = m * lax.rsqrt(v + 1e-8) + 0.1 * w
    return (w - 0.02 * step).astype(BF16), m, v


TILE = 512
FB = 256


def tiles(tokens):
    return [pl.ds(r, TILE) for r in range(0, tokens, TILE)]


def nn(a, b):
    return dot(a, b, ((1,), (0,)))


def nt(a, b):
    return dot(a, b, ((1,), (1,)))


def gates(a, wg, wu):
    gate, up = nn(a, wg), nn(a, wu)
    s = 0.5 + 0.5 * jnp.tanh(0.5 * gate)
    silu = gate * s
    return silu, up * (s + silu * (1 - s)), (silu * up).astype(BF16)


def forward_kernel(x, dy, wg, wu, wd, silu_out, slope_out, inner_out, at_out, dyt_out, h_out, a_out, a, acc):
    j = pl.program_id(0)
    tokens = x.shape[0]

    @pl.when(j == 0)
    def _():
        for r in tiles(tokens):
            a[r] = normed(x[r])[0]
            acc[r] = jnp.zeros((TILE, x.shape[1]), F32)

    part = pl.ds(pl.multiple_of(j * FB, FB), FB)
    at_out[...] = a[part].T
    dyt_out[...] = dy[part].T
    for r in tiles(tokens):
        silu, slope, inner = gates(a[r], wg[...], wu[...])
        silu_out[r], slope_out[r], inner_out[r] = silu, slope, inner
        acc[r] += nn(inner, wd[...])

    @pl.when(j == pl.num_programs(0) - 1)
    def _():
        for r in tiles(tokens):
            h = x[r] + acc[r].astype(BF16)
            h_out[r] = h
            a_out[r] = normed(h)[0]


def forward(x, dy, wg, wu, wd):
    tokens, d = x.shape
    steps = tokens // FB
    whole = lambda s: pl.BlockSpec(s, lambda j: (0, 0))
    cols = lambda rows: pl.BlockSpec((rows, FB), lambda j: (0, j))
    wcols = pl.BlockSpec((None, d, FB), lambda j: (0, 0, j))
    wrows = pl.BlockSpec((None, FB, d), lambda j: (0, j, 0))
    ff = wg.shape[2]
    shape = jax.ShapeDtypeStruct
    return pl.pallas_call(
        forward_kernel,
        grid=(ff // FB,),
        in_specs=[whole(x.shape), whole(x.shape), wcols, wcols, wrows],
        out_specs=[cols(tokens), cols(tokens), cols(tokens), cols(d), cols(d), whole(x.shape), whole(x.shape)],
        out_shape=[shape((tokens, ff), F32)] * 2
        + [shape((tokens, ff), BF16)]
        + [shape((d, tokens), BF16)] * 2
        + [shape(x.shape, BF16)] * 2,
        scratch_shapes=[pltpu.VMEM(x.shape, BF16), pltpu.VMEM(x.shape, F32)],
        compiler_params=pltpu.CompilerParams(vmem_limit_bytes=60 * 2**20),
        name="forward",
    )(x, dy, wg, wu, wd)


class Place:
    def __init__(self):
        self.me = lax.axis_index("dp")
        self.chip, self.core = lax.div(self.me, 2), lax.rem(self.me, 2)
        self.at = self.flip(self.chip)
        self.partner = self.chip * 2 + 1 - self.core

    @staticmethod
    def flip(c):
        half = CHIPS // 2
        return c + lax.div(c, half) * (3 * half - 1 - 2 * c)

    def chip_at(self, offset):
        return self.flip(lax.rem(self.at + offset + 2 * CHIPS, CHIPS))

    def device_at(self, offset):
        return self.chip_at(offset) * 2 + self.core


def remote(src, dst, send, recv, device):
    return pltpu.make_async_remote_copy(src, dst, send, recv, device_id={"dp": device}, device_id_type=MESH)


def greet(n):
    me = lax.axis_index("dp")
    barrier = pltpu.get_barrier_semaphore()

    @pl.loop(1, n)
    def _(j):
        pl.semaphore_signal(barrier, inc=1, device_id={"dp": lax.rem(me + j, n)}, device_id_type=MESH)

    pl.semaphore_wait(barrier, n - 1)


def wide(ref):
    return ref[...].astype(F32)


class Stream:
    def __init__(self, refs):
        self.own40, self.peer40, self.got40, self.stage40, self.own64, self.peer64, self.got64, self.stage64 = refs[:8]
        self.sq40, self.sq64 = refs[8:10]
        self.pair40_send, self.pair40_recv, self.pair64_send, self.pair64_recv = refs[10:14]
        self.ring40_send, self.ring40_recv, self.ring64_send, self.ring64_recv = refs[14:18]
        self.here = Place()

    def keep(self, step, gate, up, down):
        c, part = lax.div(step, 2), lax.rem(step, 2)
        slot = lax.rem(c, 2)
        first = self.here.core == 0
        cols = pl.ds(pl.multiple_of(part * FB, FB), FB)
        for kind, g in enumerate((gate, up)):
            g = g.reshape(CHIPS, 2, -1, FB)
            self.own40[kind, c, :, :, cols] = jnp.where(first, g[:, 0], g[:, 1]).astype(BF16)
            self.stage40[slot, kind, :, :, cols] = jnp.where(first, g[:, 1], g[:, 0]).astype(BF16)
        g = down.reshape(2, *self.own64.shape[2:])
        self.own64[c, part] = jnp.where(first, g[0], g[1]).astype(BF16)
        self.stage64[slot, part] = jnp.where(first, g[1], g[0]).astype(BF16)

    def pair40(self, kind, c):
        return remote(self.stage40.at[lax.rem(c, 2), kind], self.peer40.at[kind, c], self.pair40_send.at[kind, c], self.pair40_recv.at[kind, c], self.here.partner)

    def pair64(self, c):
        return remote(self.stage64.at[lax.rem(c, 2)], self.peer64.at[c], self.pair64_send.at[c], self.pair64_recv.at[c], self.here.partner)

    def swap(self, c):
        self.pair64(c).start()
        self.pair40(0, c).start()
        self.pair40(1, c).start()

    def swapped_out(self, c):
        self.pair64(c).wait_send()
        self.pair40(0, c).wait_send()
        self.pair40(1, c).wait_send()

    def hop40(self, kind, c, h):
        sign = 1 - 2 * kind
        q = self.here.chip_at(-sign * (1 + h))
        return remote(self.own40.at[kind, c, q], self.got40.at[kind, c, h], self.ring40_send.at[kind, c, h], self.ring40_recv.at[kind, c, h], self.here.device_at(sign))

    def hop64(self, c, part, side):
        return remote(self.own64.at[c, part, side], self.got64.at[c, part, side], self.ring64_send.at[c, part, side], self.ring64_recv.at[c, part, side], self.here.device_at(1 - 2 * side))

    def turn64(self, c, part, side):
        to = self.here.flip(lax.rem(2 * c + part, CHIPS))
        return lax.rem((1 - 2 * side) * (self.here.at - to) - 1 + 2 * CHIPS, CHIPS)

    def advance(self, c, h, g40, g64):
        layer, quarter = 1 - lax.div(c, 4), lax.rem(c, 4)
        here = self.here

        @pl.when(h == 0)
        def _():
            self.pair64(c).wait_recv()
            for kind in range(2):
                self.pair40(kind, c).wait_recv()
                q = here.chip_at(-(1 - 2 * kind))
                mine = self.own40.at[kind, c, q]
                mine[...] = (wide(mine) + wide(self.peer40.at[kind, c, q])).astype(BF16)
                self.hop40(kind, c, 0).start()

        @pl.when((h > 0) & (h < HOPS))
        def _():
            for kind in range(2):
                self.hop40(kind, c, h - 1).wait_recv()
                q = here.chip_at(-(1 - 2 * kind) * (1 + h))
                mine = self.own40.at[kind, c, q]
                mine[...] = (wide(mine) + wide(self.peer40.at[kind, c, q]) + wide(self.got40.at[kind, c, h - 1])).astype(BF16)
                self.hop40(kind, c, h).start()

        @pl.when(h == HOPS)
        def _():
            for kind in range(2):
                self.hop40(kind, c, HOPS - 1).wait_recv()
                q = here.chip
                g = (wide(self.own40.at[kind, c, q]) + wide(self.peer40.at[kind, c, q]) + wide(self.got40.at[kind, c, HOPS - 1])).astype(BF16)
                g40[kind, layer, :, pl.ds(pl.multiple_of(quarter * 2 * FB, 2 * FB), 2 * FB)] = g
                g = g.astype(F32)
                self.sq40[...] += g * g

        for part in range(2):
            for side in range(2):
                turn = self.turn64(c, part, side)
                mine, theirs, got = (r.at[c, part, side] for r in (self.own64, self.peer64, self.got64))

                @pl.when((h == turn) & (h == 0))
                def _():
                    mine[...] = (wide(mine) + wide(theirs)).astype(BF16)
                    self.hop64(c, part, side).start()

                @pl.when((h == turn) & (h > 0) & (h < HOPS))
                def _():
                    self.hop64(c, part, side).wait_recv()
                    mine[...] = (wide(mine) + wide(theirs) + wide(got)).astype(BF16)
                    self.hop64(c, part, side).start()

                @pl.when((h == turn) & (h == HOPS))
                def _():
                    self.hop64(c, part, side).wait_recv()
                    g = (wide(mine) + wide(theirs) + wide(got)).astype(BF16)
                    g64[layer, side] = g
                    g = g.astype(F32)
                    self.sq64[...] += g * g

    def tick(self, tick, g40, g64):
        @pl.loop(0, 8)
        def _(c):
            early = 1 - lax.div(lax.div(c, 3) + 2, 3)
            h = tick - (2 * c + 10 - early * (5 - 2 * c))

            @pl.when((h >= 0) & (h <= HOPS))
            def _():
                self.advance(c, h, g40, g64)

    def drain(self):
        self.swapped_out(6)
        self.swapped_out(7)

        @pl.loop(0, 8)
        def _(c):
            for kind in range(2):

                @pl.loop(0, HOPS)
                def _(h):
                    self.hop40(kind, c, h).wait_send()

            for part in range(2):
                for side in range(2):

                    @pl.when(self.turn64(c, part, side) < HOPS)
                    def _():
                        self.hop64(c, part, side).wait_send()


def backward_kernel(dy_in, a_in, h_in, dyt_in, a0t_in, wg, wu, wd, silu, slope, inner0, g40, g64, squares, *refs):
    d, a, dt, at, da, inner, dg, du, sems = refs[:9]
    stream = Stream(refs[9:])
    step = pl.program_id(0)
    half = pl.num_programs(0) // 2
    tokens = d.shape[0]

    def load(src, dst, i):
        return pltpu.make_async_copy(src, dst, sems.at[i])

    def gradients(inner):
        @pl.when((lax.rem(step, 2) == 0) & (step >= 4))
        def _():
            stream.swapped_out(lax.div(step, 2) - 2)

        stream.keep(step, nn(at[...], dg[...]), nn(at[...], du[...]), nn(dt[...], inner[...]).T)

        @pl.when(lax.rem(step, 2) == 1)
        def _():
            stream.swap(lax.div(step, 2))

    @pl.when(step == 0)
    def _():
        here = stream.here
        for device in (here.device_at(1), here.device_at(-1), here.partner):
            pl.semaphore_signal(pltpu.get_barrier_semaphore(), inc=1, device_id={"dp": device}, device_id_type=MESH)
        first = [load(dy_in, d, 0), load(a_in, a, 1), load(dyt_in, dt, 2)]
        for c in first:
            c.start()
        for r in tiles(tokens):
            da[r] = jnp.zeros((TILE, d.shape[1]), F32)
        stream.sq40[...] = jnp.zeros_like(stream.sq40)
        stream.sq64[...] = jnp.zeros_like(stream.sq64)
        for c in first:
            c.wait()
        at[...] = a[...].T

    @pl.when(step == 1)
    def _():
        pl.semaphore_wait(pltpu.get_barrier_semaphore(), 3)

    @pl.when(step < half)
    def _():
        stream.tick(2 * step, g40, g64)
        both = jnp.concatenate([wg[...], wu[...]], axis=1)
        for r in tiles(tokens):
            by_inner = nt(d[r], wd[...]).astype(BF16).astype(F32)
            silu, slope, product = gates(a[r], wg[...], wu[...])
            by_gate, by_up = (by_inner * slope).astype(BF16), (by_inner * silu).astype(BF16)
            inner[r], dg[r], du[r] = product, by_gate, by_up
            da[r] += nt(jnp.concatenate([by_gate, by_up], axis=1), both)
        stream.tick(2 * step + 1, g40, g64)

        @pl.when(step == half - 1)
        def _():
            load(h_in, a, 1).start()

        gradients(inner)

    @pl.when(step == half - 1)
    def _():
        c = load(a0t_in, at, 0)
        c.start()
        load(h_in, a, 1).wait()
        for r in tiles(tokens):
            h = a[r].astype(F32)
            scale = lax.rsqrt(jnp.mean(h**2, -1, keepdims=True) + 1e-6)
            by_a = da[r].astype(BF16).astype(F32)
            by_h = scale * by_a - h * (scale**3 * jnp.mean(by_a * h, -1, keepdims=True))
            d[r] = d[r] + by_h.astype(BF16)
        dt[...] = d[...].T
        c.wait()

    @pl.when(step >= half)
    def _():
        for r in tiles(tokens):
            by_inner = nt(d[r], wd[...]).astype(BF16).astype(F32)
            dg[r], du[r] = (by_inner * slope[r]).astype(BF16), (by_inner * silu[r]).astype(BF16)
        stream.tick(step + half, g40, g64)
        gradients(inner0)

    @pl.when(step == 2 * half - 1)
    def _():
        @pl.loop(0, CHIPS)
        def _(t):
            stream.tick(3 * half + t, g40, g64)

        stream.drain()
        total = jnp.sum(stream.sq40[...], keepdims=True) + jnp.sum(stream.sq64[...], keepdims=True)
        squares[...] = jnp.broadcast_to(total, squares.shape)


def backward(dy, a1, h1, dyt, a0t, wg, wu, wd, silu, slope, inner0):
    tokens, d = dy.shape
    ff = wg.shape[2]
    half = ff // FB
    early = lambda s: jnp.minimum(s, half - 1)
    late = lambda s: jnp.maximum(s - half, 0)
    layer = lambda s: 1 - s // half
    wcols = pl.BlockSpec((None, d, FB), lambda s: (1, 0, early(s)))
    wrows = pl.BlockSpec((None, FB, d), lambda s: (layer(s), s % half, 0))
    saved = pl.BlockSpec((tokens, FB), lambda s: (0, late(s)))
    rows, block = pltpu.VMEM((tokens, d), BF16), pltpu.VMEM((tokens, FB), BF16)
    flipped = pltpu.VMEM((d, tokens), BF16)
    dma = pltpu.SemaphoreType.DMA
    of40 = lambda *s: pltpu.VMEM((*s, 40, 2 * FB), BF16)
    of64 = lambda *s: pltpu.VMEM((*s, 2, 64, 640), BF16)
    comms = [of40(2, 8, CHIPS), of40(2, 8, CHIPS), of40(2, 8, HOPS), of40(2, 2, CHIPS)]
    comms += [of64(8, 2), of64(8, 2), of64(8, 2), of64(2, 2)]
    comms += [pltpu.VMEM((40, 2 * FB), F32), pltpu.VMEM((64, 640), F32)]
    comms += [dma((2, 8)), dma((2, 8)), dma((8,)), dma((8,)), dma((2, 8, HOPS)), dma((2, 8, HOPS)), dma((8, 2, 2)), dma((8, 2, 2))]
    return pl.pallas_call(
        backward_kernel,
        grid=(2 * half,),
        in_specs=[ANY] * 5 + [wcols, wcols, wrows, saved, saved, saved],
        out_specs=[pl.BlockSpec(memory_space=pltpu.VMEM)] * 3,
        out_shape=[pltpu.VMEM((2, 2, 40, ff), BF16), pltpu.VMEM((2, 2, 64, 640), BF16), pltpu.VMEM((8, 128), F32)],
        scratch_shapes=[rows, rows, flipped, flipped, pltpu.VMEM((tokens, d), F32), block, block, block, dma((3,))] + comms,
        compiler_params=pltpu.CompilerParams(collective_id=1, has_side_effects=True, vmem_limit_bytes=62 * 2**20),
        name="backward",
    )(dy, a1, h1, dyt, a0t, wg, wu, wd, silu, slope, inner0)


def comm_kernel(n, count, *refs):
    it = iter(refs)
    take = lambda k: [next(it) for _ in range(k)]
    g40, g64, own_squares = take(3)
    ws, ms, vs = take(3), take(3), take(3)
    w_out, m_out, v_out = take(3), take(3), take(3)
    w40, w64, m40, m64, v40, v64, squares, local_sem = take(8)
    sq_send, sq_recv, gat_send, gat_recv, cross_send, cross_recv = take(6)

    here = Place()
    me, core = here.me, here.core
    streams = [(layer, kind) for kind in range(4) for layer in (1, 0)]
    sign = lambda kind: 1 - 2 * (kind % 2)
    loads = []

    def load(src, dst):
        c = pltpu.make_async_copy(src, dst, local_sem.at[len(loads)])
        c.start()
        loads.append(c)

    for side, x40, x64, per in ((ws, w40, w64, True), (ms, m40, m64, False), (vs, v40, v64, False)):
        for i in range(2):
            load(side[i].at[:, me] if per else side[i], x40.at[i])
        load(side[2].at[:, me] if per else side[2], x64)

    greet(n)
    squares[me] = own_squares[...]

    def tell(j):
        return remote(squares.at[me], squares.at[me], sq_send.at[j], sq_recv.at[me], lax.rem(me + j, n))

    def told(j):
        o = lax.rem(me + n - j, n)
        return remote(squares.at[o], squares.at[o], sq_send.at[j], sq_recv.at[o], o)

    @pl.loop(1, n)
    def _(j):
        tell(j).start()

    for c in loads:
        c.wait()

    @pl.loop(1, n)
    def _(j):
        told(j).wait_recv()

    total = jnp.sum(squares[...], axis=0)[:1, :1]
    factor = jnp.minimum(1.0, 0.5 * lax.rsqrt(total / count + 1e-30))

    def whole(layer, kind, owner):
        return w_out[kind].at[layer, owner] if kind < 2 else w_out[2].at[layer, owner, kind - 2]

    def pass_on(i, layer, kind, t):
        o = here.device_at(-sign(kind) * t)
        block = whole(layer, kind, o)
        return remote(block, block, gat_send.at[i, t], gat_recv.at[i, t], here.device_at(sign(kind)))

    def across(i, layer, kind, t):
        o = here.device_at(-sign(kind) * t)
        block = whole(layer, kind, o)
        return remote(block, block, cross_send.at[i, t], cross_recv.at[i, t], here.partner)

    def across_in(i, layer, kind, t):
        o = here.chip_at(-sign(kind) * t) * 2 + 1 - core
        block = whole(layer, kind, o)
        return remote(block, block, cross_send.at[i, t], cross_recv.at[i, t], here.partner)

    for i, (layer, kind) in enumerate(streams):
        sel = (lambda r40, r64: r40.at[kind, layer] if kind < 2 else r64.at[layer, kind - 2])
        out = (lambda r: r[kind].at[layer] if kind < 2 else r[2].at[layer, kind - 2])
        g = wide(g40.at[kind, layer] if kind < 2 else g64.at[layer, kind - 2]) * factor
        w, m, v = adamw(wide(sel(w40, w64)), sel(m40, m64)[...], sel(v40, v64)[...], g)
        whole(layer, kind, me)[...] = w
        pass_on(i, layer, kind, 0).start()
        across(i, layer, kind, 0).start()
        out(m_out)[...] = m
        out(v_out)[...] = v

    @pl.loop(1, HOPS)
    def _(t):
        for i, (layer, kind) in enumerate(streams):
            pass_on(i, layer, kind, t - 1).wait_recv()
            pass_on(i, layer, kind, t).start()
            across(i, layer, kind, t).start()

    for i, (layer, kind) in enumerate(streams):
        pass_on(i, layer, kind, HOPS - 1).wait_recv()
        across(i, layer, kind, HOPS).start()

    @pl.loop(0, HOPS)
    def _(t):
        for i, (layer, kind) in enumerate(streams):
            pass_on(i, layer, kind, t).wait_send()

    @pl.loop(1, n)
    def _(j):
        tell(j).wait_send()

    @pl.loop(0, CHIPS)
    def _(t):
        for i, (layer, kind) in enumerate(streams):
            across(i, layer, kind, t).wait_send()
            across_in(i, layer, kind, t).wait_recv()


def comm(n, count, grads, ws, ms, vs):
    dma = pltpu.SemaphoreType.DMA
    scratch = [pltpu.VMEM((2, 2, 40, 2048), BF16), pltpu.VMEM((2, 2, 64, 640), BF16)]
    scratch += [pltpu.VMEM((2, 2, 40, 2048), F32), pltpu.VMEM((2, 2, 64, 640), F32)] * 2
    scratch += [pltpu.VMEM((n, 8, 128), F32), dma((9,)), dma((n,)), dma((n,))]
    scratch += [dma((8, HOPS)), dma((8, HOPS)), dma((8, CHIPS)), dma((8, CHIPS))]
    out_shape = [pltpu.VMEM((2, n, 40, 2048), BF16)] * 2 + [pltpu.VMEM((2, n, 2, 64, 640), BF16)]
    out_shape += ([pltpu.VMEM((2, 40, 2048), F32)] * 2 + [pltpu.VMEM((2, 2, 64, 640), F32)]) * 2
    return pl.pallas_call(
        lambda *refs: comm_kernel(n, count, *refs),
        out_shape=out_shape,
        in_specs=[pl.BlockSpec(memory_space=pltpu.VMEM)] * 3 + [ANY] * 9,
        out_specs=[pl.BlockSpec(memory_space=pltpu.VMEM)] * 9,
        scratch_shapes=scratch,
        compiler_params=pltpu.CompilerParams(collective_id=0, has_side_effects=True, vmem_limit_bytes=16 * 2**20),
        name="comm",
    )(*grads, *ws, *ms, *vs)


def write_kernel(*refs):
    k = (len(refs) - 1) // 2
    copies = [pltpu.make_async_copy(refs[i], refs[k + i], refs[-1].at[i]) for i in range(k)]
    for c in copies:
        c.start()
    for c in copies:
        c.wait()


def write(arrays):
    return pl.pallas_call(
        write_kernel,
        out_shape=[jax.ShapeDtypeStruct(a.shape, a.dtype) for a in arrays],
        in_specs=[pl.BlockSpec(memory_space=pltpu.VMEM)] * len(arrays),
        out_specs=[ANY] * len(arrays),
        scratch_shapes=[pltpu.SemaphoreType.DMA((len(arrays),))],
        compiler_params=pltpu.CompilerParams(vmem_limit_bytes=2**20),
        name="write",
    )(*arrays)


def solution(mesh):
    n = mesh.shape["dp"]

    def body(x, dy, wg, wu, wd, mg, mu, md, vg, vu, vd):
        x, dy = x[0], dy[0]
        silu, slope, inner0, a0t, dyt, h1, a1 = forward(x, dy, wg, wu, wd)
        grads = backward(dy, a1, h1, dyt, a0t, wg, wu, wd, silu, slope, inner0)
        rows = lambda w: w.reshape(2, n, 40, 2048)
        ws = [rows(wg), rows(wu), wd.reshape(2, n, 2, 64, 640)]
        split = lambda t: t.reshape(2, 2, 64, 640)
        count = wg.size + wu.size + wd.size
        outs = write(comm(n, count, grads, ws, [mg, mu, split(md)], [vg, vu, split(vd)]))
        shapes = [wg, wu, wd, mg, mu, md, vg, vu, vd]
        return tuple(o.reshape(s.shape) for o, s in zip(outs, shapes, strict=True))

    whole, mine = P(), P(None, "dp", None)
    seq, out = P(("rep", "dp")), P("rep", "dp", None)
    return jax.shard_map(
        body,
        mesh=mesh,
        in_specs=(seq, seq) + (whole,) * 3 + (mine,) * 6,
        out_specs=(P("rep"),) * 3 + (out,) * 6,
        check_vma=False,
    )
```

```python
import jax
import jax.numpy as jnp
from jax import lax
from jax.experimental import pallas as pl
from jax.experimental.pallas import tpu as pltpu
from jax.sharding import PartitionSpec as P

F32, BF16 = jnp.float32, jnp.bfloat16
MESH = pl.DeviceIdType.MESH
ANY = pl.BlockSpec(memory_space=pl.ANY)
CHIPS = 8
HOPS = CHIPS - 1


def dot(a, b, dims):
    return lax.dot_general(a, b, (dims, ((), ())), preferred_element_type=F32)


def normed(h):
    wide = h.astype(F32)
    scale = lax.rsqrt(jnp.mean(wide**2, -1, keepdims=True) + 1e-6)
    return (wide * scale).astype(BF16), scale


def adamw(w, m, v, g):
    m = 0.9 * m + 0.1 * g
    v = 0.95 * v + 0.05 * g * g
    step = m * lax.rsqrt(v + 1e-8) + 0.1 * w
    return (w - 0.02 * step).astype(BF16), m, v


TILE = 512
FB = 256
WIDE = 512
LAST = 1
ROW = 4
MIB = 2**20


def tiles(tokens):
    return [pl.ds(r, TILE) for r in range(0, tokens, TILE)]


def nn(a, b):
    return dot(a, b, ((1,), (0,)))


def nt(a, b):
    return dot(a, b, ((1,), (1,)))


def gates(a, wg, wu):
    gate, up = nn(a, wg), nn(a, wu)
    s = 0.5 + 0.5 * jnp.tanh(0.5 * gate)
    silu = gate * s
    return silu, up * (s + silu * (1 - s)), (silu * up).astype(BF16)


def forward_kernel(x, dy, wg, wu, wd, silu_out, slope_out, inner_out, at_out, dyt_out, h_out, a_out, a, acc):
    j = pl.program_id(0)
    tokens = x.shape[0]

    @pl.when(j == 0)
    def _():
        for r in tiles(tokens):
            a[r] = normed(x[r])[0]
            acc[r] = jnp.zeros((TILE, x.shape[1]), F32)

    part = pl.ds(pl.multiple_of(j * WIDE, WIDE), WIDE)
    at_out[...] = a[part].T
    dyt_out[...] = dy[part].T
    for r in tiles(tokens):
        silu, slope, inner = gates(a[r], wg[...], wu[...])
        silu_out[r], slope_out[r], inner_out[r] = silu, slope, inner
        acc[r] += nn(inner, wd[...])

    @pl.when(j == pl.num_programs(0) - 1)
    def _():
        for r in tiles(tokens):
            h = x[r] + acc[r].astype(BF16)
            h_out[r] = h
            a_out[r] = normed(h)[0]


def forward(x, dy, wg, wu, wd):
    tokens, d = x.shape
    whole = lambda s: pl.BlockSpec(s, lambda j: (0, 0))
    cols = lambda rows: pl.BlockSpec((rows, WIDE), lambda j: (0, j))
    wcols = pl.BlockSpec((None, d, WIDE), lambda j: (0, 0, j))
    wrows = pl.BlockSpec((None, WIDE, d), lambda j: (0, j, 0))
    ff = wg.shape[2]
    shape = jax.ShapeDtypeStruct
    return pl.pallas_call(
        forward_kernel,
        grid=(ff // WIDE,),
        in_specs=[whole(x.shape), whole(x.shape), wcols, wcols, wrows],
        out_specs=[cols(tokens), cols(tokens), cols(tokens), cols(d), cols(d), whole(x.shape), whole(x.shape)],
        out_shape=[shape((tokens, ff), F32)] * 2
        + [shape((tokens, ff), BF16)]
        + [shape((d, tokens), BF16)] * 2
        + [shape(x.shape, BF16)] * 2,
        scratch_shapes=[pltpu.VMEM(x.shape, BF16), pltpu.VMEM(x.shape, F32)],
        compiler_params=pltpu.CompilerParams(vmem_limit_bytes=60 * MIB),
        name="forward",
    )(x, dy, wg, wu, wd)


class Place:
    def __init__(self):
        self.me = lax.axis_index("dp")
        self.chip, self.core = lax.div(self.me, 2), lax.rem(self.me, 2)
        self.at = self.flip(self.chip)
        self.partner = self.chip * 2 + 1 - self.core

    @staticmethod
    def flip(c):
        half = CHIPS // 2
        return c + lax.div(c, half) * (3 * half - 1 - 2 * c)

    def chip_at(self, offset):
        return self.flip(lax.rem(self.at + offset + 2 * CHIPS, CHIPS))

    def device_at(self, offset):
        return self.chip_at(offset) * 2 + self.core


def remote(src, dst, send, recv, device):
    return pltpu.make_async_remote_copy(src, dst, send, recv, device_id={"dp": device}, device_id_type=MESH)


def greet(n):
    me = lax.axis_index("dp")
    barrier = pltpu.get_barrier_semaphore()

    @pl.loop(1, n)
    def _(j):
        pl.semaphore_signal(barrier, inc=1, device_id={"dp": lax.rem(me + j, n)}, device_id_type=MESH)

    pl.semaphore_wait(barrier, n - 1)


def wide(ref):
    return ref[...].astype(F32)


class Stream:
    def __init__(self, refs):
        self.own40, self.peer40, self.across40, self.along40, self.stage40 = refs[:5]
        self.own64, self.peer64, self.across64, self.along64, self.stage64 = refs[5:10]
        self.sq40, self.sq64, self.both64 = refs[10:13]
        self.sems = dict(zip(("pair40", "pair64", "y40", "y64", "z40", "z64", "far40", "far64"), zip(refs[13::2], refs[14::2])))
        self.me = lax.axis_index("dp")
        self.chip, self.core = lax.div(self.me, 2), lax.rem(self.me, 2)
        self.y, self.z = lax.div(self.chip, ROW), lax.rem(self.chip, ROW)
        self.partner = self.device(self.y, self.z, 1 - self.core)
        self.facing = self.device(1 - self.y, self.z, self.core)
        self.mate_z = self.z + 1 - 2 * lax.rem(self.z, 2)
        self.mate, self.far = self.device(self.y, self.mate_z, self.core), self.device(self.y, 3 - self.z, self.core)

    @staticmethod
    def device(y, z, core):
        return (y * ROW + z) * 2 + core

    def copy(self, name, src, dst, send, recv, device):
        out, into = self.sems[name]
        return remote(src, dst, out.at[send], into.at[recv], device)

    def keep40(self, c, part, gate, up):
        first = self.core == 0
        cols = pl.ds(pl.multiple_of(part * FB, FB), FB)
        for kind, g in enumerate((gate, up)):
            g = g.reshape(CHIPS, 2, -1, FB)
            self.own40[c, :, kind, :, cols] = jnp.where(first, g[:, 0], g[:, 1]).astype(BF16)
            self.stage40[lax.rem(c, 2), :, kind, :, cols] = jnp.where(first, g[:, 1], g[:, 0]).astype(BF16)

    def keep64(self, c, part, down):
        first = self.core == 0
        g = down.reshape(2, *self.own64.shape[2:])
        self.own64[c, part] = jnp.where(first, g[0], g[1]).astype(BF16)
        self.stage64[lax.rem(c, 2), part] = jnp.where(first, g[1], g[0]).astype(BF16)

    def pair40(self, c):
        return self.copy("pair40", self.stage40.at[lax.rem(c, 2)], self.peer40.at[c], c, c, self.partner)

    def pair64(self, c):
        return self.copy("pair64", self.stage64.at[lax.rem(c, 2)], self.peer64.at[c], c, c, self.partner)

    def y40(self, c):
        return self.copy("y40", self.own40.at[c, pl.ds((1 - self.y) * ROW, 4)], self.across40.at[c], c, c, self.facing)

    def y64(self, c):
        return self.copy("y64", self.own64.at[c, 1 - self.y], self.across64.at[c], c, c, self.facing)

    def z40(self, c, i):
        to = (self.mate_z, 3 - self.mate_z)[i]
        return self.copy("z40", self.own40.at[c, self.y * ROW + to], self.along40.at[c, i], (c, i), (c, i), self.mate)

    def far40(self, c):
        return self.copy("far40", self.own40.at[c, self.y * ROW + 3 - self.z], self.along40.at[c, 2], c, c, self.far)

    def z64(self, c, i):
        return self.copy("z64", self.own64.at[c, self.y], self.along64.at[i], (0, i), (0, i), self.mate)

    def far64(self, c):
        return self.copy("far64", self.own64.at[c, self.y], self.along64.at[2], 0, 0, self.far)

    def first_copy(self, c, i):
        at = (LAST, i)
        return self.copy("z64", self.own64.at[c], self.both64.at[i], at, at, self.mate)

    def second_copy(self, c):
        return self.copy("far64", self.own64.at[c], self.both64.at[2], LAST, LAST, self.far)

    def pair_sum(self, c, row):
        return wide(self.own64.at[c, row]) + wide(self.peer64.at[c, row])

    def row_sum(self, c, row):
        return self.pair_sum(c, row) + wide(self.both64.at[0, row]) + wide(self.both64.at[2, row])

    def first64(self, c):
        self.pair64(c).wait_recv()
        for i, owner in enumerate((self.mate_z, 3 - self.mate_z)):

            @pl.when(owner == lax.rem(c, ROW))
            def _():
                for row in range(2):
                    self.own64[c, row] = self.pair_sum(c, row).astype(BF16)
                self.first_copy(c, i).start()

    def second64(self, c):
        @pl.when(3 - self.z == lax.rem(c, ROW))
        def _():
            self.first_copy(c, 1).wait_recv()
            for row in range(2):
                self.own64[c, row] = (self.pair_sum(c, row) + wide(self.both64.at[1, row])).astype(BF16)
            self.second_copy(c).start()

    def third64(self):
        c = ROW + self.z
        self.first_copy(c, 0).wait_recv()
        self.second_copy(c).wait_recv()
        self.own64[c, 1 - self.y] = self.row_sum(c, 1 - self.y).astype(BF16)
        self.y64(c).start()

    def last64(self, g64):
        c = ROW + self.z
        self.y64(c).wait_recv()
        total = (self.row_sum(c, self.y) + wide(self.across64.at[c])).astype(BF16)
        g64[0] = total
        total = total.astype(F32)
        self.sq64[...] += total * total

    def over40(self, c):
        self.pair40(c).wait_recv()

        @pl.loop(0, ROW)
        def _(z):
            q = (1 - self.y) * ROW + z
            mine = self.own40.at[c, q]
            mine[...] = (wide(mine) + wide(self.peer40.at[c, q])).astype(BF16)

        self.y40(c).start()

    def over64(self, c):
        self.pair64(c).wait_recv()
        mine = self.own64.at[c, 1 - self.y]
        mine[...] = (wide(mine) + wide(self.peer64.at[c, 1 - self.y])).astype(BF16)
        self.y64(c).start()

    def sum40(self, c, z):
        q = self.y * ROW + z
        return wide(self.own40.at[c, q]) + wide(self.peer40.at[c, q]) + wide(self.across40.at[c, z])

    def sum64(self, c):
        return wide(self.own64.at[c, self.y]) + wide(self.peer64.at[c, self.y]) + wide(self.across64.at[c])

    def on40(self, c):
        self.y40(c).wait_recv()
        for i, to in enumerate((self.mate_z, 3 - self.mate_z)):
            self.own40[c, self.y * ROW + to] = self.sum40(c, to).astype(BF16)
            self.z40(c, i).start()

    def on64(self, c):
        self.y64(c).wait_recv()
        for i, owner in enumerate((self.mate_z, 3 - self.mate_z)):

            @pl.when(owner == lax.rem(c, ROW))
            def _():
                self.own64[c, self.y] = self.sum64(c).astype(BF16)
                self.z64(c, i).start()

    def out40(self, c):
        self.z40(c, 1).wait_recv()
        to = 3 - self.z
        self.own40[c, self.y * ROW + to] = (self.sum40(c, to) + wide(self.along40.at[c, 1])).astype(BF16)
        self.far40(c).start()

    def out64(self, c):
        @pl.when(3 - self.z == lax.rem(c, ROW))
        def _():
            self.z64(c, 1).wait_recv()
            self.own64[c, self.y] = (self.sum64(c) + wide(self.along64.at[1])).astype(BF16)
            self.far64(c).start()

    def end40(self, c, g40):
        self.z40(c, 0).wait_recv()
        self.far40(c).wait_recv()
        total = (self.sum40(c, self.z) + wide(self.along40.at[c, 0]) + wide(self.along40.at[c, 2])).astype(BF16)
        for part in range(2):
            cols = pl.ds(pl.multiple_of((lax.rem(c, ROW) + 4 * part) * FB, FB), FB)
            g40[:, 1 - lax.div(c, ROW), :, cols] = total[:, :, part * FB : (part + 1) * FB]
        total = total.astype(F32)
        self.sq40[...] += total * total

    def end64(self, c, g64):
        @pl.when(self.z == lax.rem(c, ROW))
        def _():
            self.z64(c, 0).wait_recv()
            self.far64(c).wait_recv()
            total = (self.sum64(c) + wide(self.along64.at[0]) + wide(self.along64.at[2])).astype(BF16)
            g64[1] = total
            total = total.astype(F32)
            self.sq64[...] += total * total

    def drain(self):
        for c in (6, 7):
            self.pair40(c).wait_send()
            self.pair64(c).wait_send()

        @pl.loop(0, 8)
        def _(c):
            self.far40(c).wait_send()
            self.y40(c).wait_send()
            for i in range(2):
                self.z40(c, i).wait_send()

        @pl.loop(0, ROW)
        def _(c):
            self.y64(c).wait_send()

        self.y64(ROW + self.z).wait_send()
        self.far64(0).wait_send()
        self.second_copy(4).wait_send()
        for i in range(2):
            self.z64(0, i).wait_send()
            self.first_copy(4, i).wait_send()


def backward_kernel(dy_in, a_in, h_in, dyt_in, a0t_in, wg, wu, wd, silu, slope, inner0, g40, g64, squares, *refs):
    d, a, dt, at, da, inner, dg, du, sems = refs[:9]
    stream = Stream(refs[9:])
    step = pl.program_id(0)
    half = pl.num_programs(0) // 3
    tokens = d.shape[0]

    def load(src, dst, i):
        return pltpu.make_async_copy(src, dst, sems.at[i])

    part, block = lax.rem(step, 2), lax.rem(lax.div(step, 2), 4)

    def gate_up(c):
        @pl.when((part == 0) & (c >= 2))
        def _():
            stream.pair40(c - 2).wait_send()

        stream.keep40(c, part, nn(at[...], dg[...]), nn(at[...], du[...]))

        @pl.when(part == 1)
        def _():
            stream.pair40(c).start()

    def down(c, inner):
        @pl.when((part == 0) & (c >= 2))
        def _():
            stream.pair64(c - 2).wait_send()

        stream.keep64(c, part, nn(dt[...], inner[...]).T)

        @pl.when(part == 1)
        def _():
            stream.pair64(c).start()

    @pl.when(step == 0)
    def _():
        for device in (stream.mate, stream.far, stream.partner, stream.facing):
            pl.semaphore_signal(pltpu.get_barrier_semaphore(), inc=1, device_id={"dp": device}, device_id_type=MESH)
        first = [load(dy_in, d, 0), load(a_in, a, 1), load(dyt_in, dt, 2)]
        for c in first:
            c.start()
        for r in tiles(tokens):
            da[r] = jnp.zeros((TILE, d.shape[1]), F32)
        stream.sq40[...] = jnp.zeros_like(stream.sq40)
        stream.sq64[...] = jnp.zeros_like(stream.sq64)
        for c in first:
            c.wait()
        at[...] = a[...].T

    @pl.when(step == 1)
    def _():
        pl.semaphore_wait(pltpu.get_barrier_semaphore(), 4)

    @pl.when(step < half)
    def _():
        both = jnp.concatenate([wg[...], wu[...]], axis=1)
        for r in tiles(tokens):
            by_inner = nt(d[r], wd[...]).astype(BF16).astype(F32)
            silu, slope, product = gates(a[r], wg[...], wu[...])
            by_gate, by_up = (by_inner * slope).astype(BF16), (by_inner * silu).astype(BF16)
            inner[r], dg[r], du[r] = product, by_gate, by_up
            da[r] += nt(jnp.concatenate([by_gate, by_up], axis=1), both)
        c = lax.div(step, 2) - 1

        @pl.when((part == 0) & (c >= 0))
        def _():
            stream.over64(c)
            stream.over40(c)

        @pl.when((part == 1) & (c >= 0))
        def _():
            stream.on64(c)
            stream.on40(c)

        @pl.when((part == 0) & (c >= 1))
        def _():
            stream.out64(c - 1)
            stream.out40(c - 1)

        @pl.when((part == 0) & (c >= 2))
        def _():
            stream.end64(c - 2, g64)
            stream.end40(c - 2, g40)

        @pl.when(step == half - 1)
        def _():
            load(h_in, a, 1).start()

        down(block, inner)
        gate_up(block)

    @pl.when(step == half - 1)
    def _():
        c = load(a0t_in, at, 0)
        c.start()
        load(h_in, a, 1).wait()
        for r in tiles(tokens):
            h = a[r].astype(F32)
            scale = lax.rsqrt(jnp.mean(h**2, -1, keepdims=True) + 1e-6)
            by_a = da[r].astype(BF16).astype(F32)
            by_h = scale * by_a - h * (scale**3 * jnp.mean(by_a * h, -1, keepdims=True))
            d[r] = d[r] + by_h.astype(BF16)
        dt[...] = d[...].T
        c.wait()

    @pl.when((step >= half) & (step < 2 * half))
    def _():
        @pl.when(step == half)
        def _():
            stream.out64(2)
            stream.out40(2)

        @pl.when(step == half + 1)
        def _():
            stream.over64(3)
            stream.over40(3)

        @pl.when(step == half + 2)
        def _():
            stream.end64(1, g64)
            stream.end40(1, g40)

        @pl.when((part == 1) & (block >= 1))
        def _():
            stream.first64(3 + block)

        @pl.when(step == half + 5)
        def _():
            stream.on64(3)
            stream.on40(3)

        down(ROW + block, inner0)

    @pl.when(step >= 2 * half)
    def _():
        for r in tiles(tokens):
            by_inner = nt(d[r], wd[...]).astype(BF16).astype(F32)
            dg[r], du[r] = (by_inner * slope[r]).astype(BF16), (by_inner * silu[r]).astype(BF16)

        @pl.when(step == 2 * half)
        def _():
            stream.first64(7)
            stream.end64(2, g64)
            stream.end40(2, g40)

        @pl.when((block >= 1) & (part == 0))
        def _():
            stream.over40(3 + block)

        @pl.when(step == 2 * half + 1)
        def _():
            stream.out64(3)
            stream.out40(3)

        @pl.when((step > 2 * half + 2) & (step <= 2 * half + 6))
        def _():
            stream.second64(1 + step - 2 * half)

        @pl.when(step == 2 * half + 5)
        def _():
            stream.end64(3, g64)
            stream.end40(3, g40)

        @pl.when((block >= 2) & (part == 1))
        def _():
            stream.on40(2 + block)

        gate_up(ROW + block)

    @pl.when(step == 3 * half - 1)
    def _():
        stream.over40(7)
        stream.out40(4)
        stream.on40(6)

        stream.third64()
        stream.out40(5)
        stream.end40(4, g40)
        stream.on40(7)
        stream.out40(6)
        stream.end40(5, g40)
        stream.last64(g64)
        stream.out40(7)
        stream.end40(6, g40)
        stream.end40(7, g40)
        stream.drain()
        total = jnp.sum(jnp.sum(stream.sq40[...], axis=0), keepdims=True) + jnp.sum(stream.sq64[...], keepdims=True)
        squares[...] = jnp.broadcast_to(total, squares.shape)


def backward(dy, a1, h1, dyt, a0t, wg, wu, wd, silu, slope, inner0):
    tokens, d = dy.shape
    ff = wg.shape[2]
    half = ff // FB
    early = lambda s: jnp.minimum(s, half - 1)
    late = lambda s: jnp.maximum(s - 2 * half, 0)
    middle = lambda s: jnp.clip(s - half, 0, half - 1)
    turn = lambda s: s // 2 + half // 2 * (s % 2)
    wcols = pl.BlockSpec((None, d, FB), lambda s: (1, 0, turn(early(s))))
    wrows = pl.BlockSpec((None, FB, d), lambda s: (1 - jnp.minimum(s // half, 1), turn(jnp.where(s < half, s, late(s))), 0))
    saved = pl.BlockSpec((tokens, FB), lambda s: (0, turn(late(s))))
    product = pl.BlockSpec((tokens, FB), lambda s: (0, turn(middle(s))))
    rows, block = pltpu.VMEM((tokens, d), BF16), pltpu.VMEM((tokens, FB), BF16)
    flipped = pltpu.VMEM((d, tokens), BF16)
    dma = pltpu.SemaphoreType.DMA
    of40 = lambda *s: pltpu.VMEM((*s, 2, 40, 2 * FB), BF16)
    of64 = lambda *s: pltpu.VMEM((*s, 128, 640), BF16)
    comms = [of40(8, CHIPS), of40(8, CHIPS), of40(8, 4), of40(8, 3), of40(2, CHIPS)]
    comms += [of64(8, 2), of64(8, 2), of64(8), of64(3), of64(2, 2)]
    comms += [pltpu.VMEM((2, 40, 2 * FB), F32), pltpu.VMEM((128, 640), F32), of64(3, 2)]
    comms += [dma((8,))] * 8 + [dma((8, 2))] * 2 + [dma((2, 2))] * 2 + [dma((8,))] * 2 + [dma((2,))] * 2
    return pl.pallas_call(
        backward_kernel,
        grid=(3 * half,),
        in_specs=[ANY] * 5 + [wcols, wcols, wrows, saved, saved, product],
        out_specs=[pl.BlockSpec(memory_space=pltpu.VMEM)] * 3,
        out_shape=[pltpu.VMEM((2, 2, 40, ff), BF16), pltpu.VMEM((2, 128, 640), BF16), pltpu.VMEM((8, 128), F32)],
        scratch_shapes=[rows, rows, flipped, flipped, pltpu.VMEM((tokens, d), F32), block, block, block, dma((3,))] + comms,
        compiler_params=pltpu.CompilerParams(collective_id=1, has_side_effects=True, vmem_limit_bytes=62 * MIB),
        name="backward",
    )(dy, a1, h1, dyt, a0t, wg, wu, wd, silu, slope, inner0)


def comm_kernel(n, count, *refs):
    it = iter(refs)
    take = lambda k: [next(it) for _ in range(k)]
    g40, g64, own_squares = take(3)
    ws, ms, vs = take(3), take(3), take(3)
    w_out, m_out, v_out = take(3), take(3), take(3)
    w40, w64, m40, m64, v40, v64, squares, local_sem = take(8)
    sq_send, sq_recv, gat_send, gat_recv, cross_send, cross_recv = take(6)

    here = Place()
    me, core = here.me, here.core
    streams = [(layer, kind) for kind in range(4) for layer in (1, 0)]
    sign = lambda kind: 1 - 2 * (kind % 2)
    loads = []

    def load(src, dst):
        c = pltpu.make_async_copy(src, dst, local_sem.at[len(loads)])
        c.start()
        loads.append(c)

    for side, x40, x64, per in ((ws, w40, w64, True), (ms, m40, m64, False), (vs, v40, v64, False)):
        for i in range(2):
            load(side[i].at[:, me] if per else side[i], x40.at[i])
        load(side[2].at[:, me] if per else side[2], x64)

    greet(n)
    squares[me] = own_squares[...]

    def tell(j):
        return remote(squares.at[me], squares.at[me], sq_send.at[j], sq_recv.at[me], lax.rem(me + j, n))

    def told(j):
        o = lax.rem(me + n - j, n)
        return remote(squares.at[o], squares.at[o], sq_send.at[j], sq_recv.at[o], o)

    @pl.loop(1, n)
    def _(j):
        tell(j).start()

    for c in loads:
        c.wait()

    @pl.loop(1, n)
    def _(j):
        told(j).wait_recv()

    total = jnp.sum(squares[...], axis=0)[:1, :1]
    factor = jnp.minimum(1.0, 0.5 * lax.rsqrt(total / count + 1e-30))

    def whole(layer, kind, owner):
        return w_out[kind].at[layer, owner] if kind < 2 else w_out[2].at[layer, owner, kind - 2]

    def pass_on(i, layer, kind, t):
        o = here.device_at(-sign(kind) * t)
        block = whole(layer, kind, o)
        return remote(block, block, gat_send.at[i, t], gat_recv.at[i, t], here.device_at(sign(kind)))

    def across(i, layer, kind, t):
        o = here.device_at(-sign(kind) * t)
        block = whole(layer, kind, o)
        return remote(block, block, cross_send.at[i, t], cross_recv.at[i, t], here.partner)

    def across_in(i, layer, kind, t):
        o = here.chip_at(-sign(kind) * t) * 2 + 1 - core
        block = whole(layer, kind, o)
        return remote(block, block, cross_send.at[i, t], cross_recv.at[i, t], here.partner)

    for i, (layer, kind) in enumerate(streams):
        sel = (lambda r40, r64: r40.at[kind, layer] if kind < 2 else r64.at[layer, kind - 2])
        out = (lambda r: r[kind].at[layer] if kind < 2 else r[2].at[layer, kind - 2])
        g = wide(g40.at[kind, layer] if kind < 2 else g64.at[layer, pl.ds((kind - 2) * 64, 64)]) * factor
        w, m, v = adamw(wide(sel(w40, w64)), sel(m40, m64)[...], sel(v40, v64)[...], g)
        whole(layer, kind, me)[...] = w
        pass_on(i, layer, kind, 0).start()
        across(i, layer, kind, 0).start()
        out(m_out)[...] = m
        out(v_out)[...] = v

    @pl.loop(1, HOPS)
    def _(t):
        for i, (layer, kind) in enumerate(streams):
            pass_on(i, layer, kind, t - 1).wait_recv()
            pass_on(i, layer, kind, t).start()
            across(i, layer, kind, t).start()

    for i, (layer, kind) in enumerate(streams):
        pass_on(i, layer, kind, HOPS - 1).wait_recv()
        across(i, layer, kind, HOPS).start()

    @pl.loop(0, HOPS)
    def _(t):
        for i, (layer, kind) in enumerate(streams):
            pass_on(i, layer, kind, t).wait_send()

    @pl.loop(1, n)
    def _(j):
        tell(j).wait_send()

    @pl.loop(0, CHIPS)
    def _(t):
        for i, (layer, kind) in enumerate(streams):
            across(i, layer, kind, t).wait_send()
            across_in(i, layer, kind, t).wait_recv()


def comm(n, count, grads, ws, ms, vs):
    dma = pltpu.SemaphoreType.DMA
    scratch = [pltpu.VMEM((2, 2, 40, 2048), BF16), pltpu.VMEM((2, 2, 64, 640), BF16)]
    scratch += [pltpu.VMEM((2, 2, 40, 2048), F32), pltpu.VMEM((2, 2, 64, 640), F32)] * 2
    scratch += [pltpu.VMEM((n, 8, 128), F32), dma((9,)), dma((n,)), dma((n,))]
    scratch += [dma((8, HOPS)), dma((8, HOPS)), dma((8, CHIPS)), dma((8, CHIPS))]
    out_shape = [pltpu.VMEM((2, n, 40, 2048), BF16)] * 2 + [pltpu.VMEM((2, n, 2, 64, 640), BF16)]
    out_shape += [pltpu.VMEM(a.shape, F32) for a in (*ms, *vs)]
    return pl.pallas_call(
        lambda *refs: comm_kernel(n, count, *refs),
        out_shape=out_shape,
        in_specs=[pl.BlockSpec(memory_space=pltpu.VMEM)] * 3 + [ANY] * 9,
        out_specs=[pl.BlockSpec(memory_space=pltpu.VMEM)] * 9,
        scratch_shapes=scratch,
        compiler_params=pltpu.CompilerParams(collective_id=0, has_side_effects=True, vmem_limit_bytes=40 * MIB),
        name="comm",
    )(*grads, *ws, *ms, *vs)


def write_kernel(*refs):
    k = (len(refs) - 1) // 2
    copies = [pltpu.make_async_copy(refs[i], refs[k + i], refs[-1].at[i]) for i in range(k)]
    for c in copies:
        c.start()
    for c in copies:
        c.wait()


def write(arrays):
    return pl.pallas_call(
        write_kernel,
        out_shape=[jax.ShapeDtypeStruct(a.shape, a.dtype) for a in arrays],
        in_specs=[pl.BlockSpec(memory_space=pltpu.VMEM)] * len(arrays),
        out_specs=[ANY] * len(arrays),
        scratch_shapes=[pltpu.SemaphoreType.DMA((len(arrays),))],
        compiler_params=pltpu.CompilerParams(vmem_limit_bytes=MIB),
        name="write",
    )(*arrays)


def solution(mesh):
    n = mesh.shape["dp"]

    def body(x, dy, wg, wu, wd, mg, mu, md, vg, vu, vd):
        x, dy = x[0], dy[0]
        silu, slope, inner0, a0t, dyt, h1, a1 = forward(x, dy, wg, wu, wd)
        grads = backward(dy, a1, h1, dyt, a0t, wg, wu, wd, silu, slope, inner0)
        rows = lambda w: w.reshape(w.shape[0], n, -1, w.shape[2])
        ws = [rows(wg), rows(wu), wd.reshape(2, n, 2, 64, 640)]
        split = lambda t: t.reshape(2, 2, 64, 640)
        count = wg.size + wu.size + wd.size
        outs = write(comm(n, count, grads, ws, [mg, mu, split(md)], [vg, vu, split(vd)]))
        shapes = [wg, wu, wd, mg, mu, md, vg, vu, vd]
        return tuple(o.reshape(s.shape) for o, s in zip(outs, shapes, strict=True))

    whole, mine = P(), P(None, "dp", None)
    seq, out = P(("rep", "dp")), P("rep", "dp", None)
    return jax.shard_map(
        body,
        mesh=mesh,
        in_specs=(seq, seq) + (whole,) * 3 + (mine,) * 6,
        out_specs=(P("rep"),) * 3 + (out,) * 6,
        check_vma=False,
    )
```

```python
import jax
import jax.numpy as jnp
from jax import lax
from jax.experimental import pallas as pl
from jax.experimental.pallas import tpu as pltpu
from jax.sharding import PartitionSpec as P

F32, BF16 = jnp.float32, jnp.bfloat16
MESH = pl.DeviceIdType.MESH
ANY = pl.BlockSpec(memory_space=pl.ANY)
CHIPS = 8
HOPS = CHIPS - 1


def dot(a, b, dims):
    return lax.dot_general(a, b, (dims, ((), ())), preferred_element_type=F32)


def normed(h):
    wide = h.astype(F32)
    scale = lax.rsqrt(jnp.mean(wide**2, -1, keepdims=True) + 1e-6)
    return (wide * scale).astype(BF16), scale


def adamw(w, m, v, g):
    m = 0.9 * m + 0.1 * g
    v = 0.95 * v + 0.05 * g * g
    step = m * lax.rsqrt(v + 1e-8) + 0.1 * w
    return (w - 0.02 * step).astype(BF16), m, v


TILE = 512
FB = 256
WIDE = 512
LAST = 1
ROW = 4
MIB = 2**20


def tiles(tokens):
    return [pl.ds(r, TILE) for r in range(0, tokens, TILE)]


def nn(a, b):
    return dot(a, b, ((1,), (0,)))


def nt(a, b):
    return dot(a, b, ((1,), (1,)))


def gates(a, wg, wu):
    gate, up = nn(a, wg), nn(a, wu)
    s = 0.5 + 0.5 * jnp.tanh(0.5 * gate)
    silu = gate * s
    return silu, up * (s + silu * (1 - s)), (silu * up).astype(BF16)


def forward_kernel(x, dy, wg, wu, wd, silu_out, slope_out, inner_out, at_out, dyt_out, h_out, a_out, a, acc):
    j = pl.program_id(0)
    tokens = x.shape[0]

    @pl.when(j == 0)
    def _():
        for r in tiles(tokens):
            a[r] = normed(x[r])[0]
            acc[r] = jnp.zeros((TILE, x.shape[1]), F32)

    part = pl.ds(pl.multiple_of(j * WIDE, WIDE), WIDE)
    at_out[...] = a[part].T
    dyt_out[...] = dy[part].T
    for r in tiles(tokens):
        silu, slope, inner = gates(a[r], wg[...], wu[...])
        silu_out[r], slope_out[r], inner_out[r] = silu, slope, inner
        acc[r] += nn(inner, wd[...])

    @pl.when(j == pl.num_programs(0) - 1)
    def _():
        for r in tiles(tokens):
            h = x[r] + acc[r].astype(BF16)
            h_out[r] = h
            a_out[r] = normed(h)[0]


def forward(x, dy, wg, wu, wd):
    tokens, d = x.shape
    whole = lambda s: pl.BlockSpec(s, lambda j: (0, 0))
    cols = lambda rows: pl.BlockSpec((rows, WIDE), lambda j: (0, j))
    wcols = pl.BlockSpec((None, d, WIDE), lambda j: (0, 0, j))
    wrows = pl.BlockSpec((None, WIDE, d), lambda j: (0, j, 0))
    ff = wg.shape[2]
    shape = jax.ShapeDtypeStruct
    return pl.pallas_call(
        forward_kernel,
        grid=(ff // WIDE,),
        in_specs=[whole(x.shape), whole(x.shape), wcols, wcols, wrows],
        out_specs=[cols(tokens), cols(tokens), cols(tokens), cols(d), cols(d), whole(x.shape), whole(x.shape)],
        out_shape=[shape((tokens, ff), F32)] * 2
        + [shape((tokens, ff), BF16)]
        + [shape((d, tokens), BF16)] * 2
        + [shape(x.shape, BF16)] * 2,
        scratch_shapes=[pltpu.VMEM(x.shape, BF16), pltpu.VMEM(x.shape, F32)],
        compiler_params=pltpu.CompilerParams(vmem_limit_bytes=60 * MIB),
        name="forward",
    )(x, dy, wg, wu, wd)


class Place:
    def __init__(self):
        self.me = lax.axis_index("dp")
        self.chip, self.core = lax.div(self.me, 2), lax.rem(self.me, 2)
        self.at = self.flip(self.chip)
        self.partner = self.chip * 2 + 1 - self.core

    @staticmethod
    def flip(c):
        half = CHIPS // 2
        return c + lax.div(c, half) * (3 * half - 1 - 2 * c)

    def chip_at(self, offset):
        return self.flip(lax.rem(self.at + offset + 2 * CHIPS, CHIPS))

    def device_at(self, offset):
        return self.chip_at(offset) * 2 + self.core


def remote(src, dst, send, recv, device):
    return pltpu.make_async_remote_copy(src, dst, send, recv, device_id={"dp": device}, device_id_type=MESH)


def greet(n):
    me = lax.axis_index("dp")
    barrier = pltpu.get_barrier_semaphore()

    @pl.loop(1, n)
    def _(j):
        pl.semaphore_signal(barrier, inc=1, device_id={"dp": lax.rem(me + j, n)}, device_id_type=MESH)

    pl.semaphore_wait(barrier, n - 1)


def wide(ref):
    return ref[...].astype(F32)


class Stream:
    def __init__(self, refs):
        self.own40, self.peer40, self.across40, self.along40, self.stage40 = refs[:5]
        self.own64, self.peer64, self.across64, self.along64, self.stage64 = refs[5:10]
        self.sq40, self.sq64, self.both64 = refs[10:13]
        self.sems = dict(zip(("pair40", "pair64", "y40", "y64", "z40", "z64", "far40", "far64"), zip(refs[13::2], refs[14::2])))
        self.me = lax.axis_index("dp")
        self.chip, self.core = lax.div(self.me, 2), lax.rem(self.me, 2)
        self.y, self.z = lax.div(self.chip, ROW), lax.rem(self.chip, ROW)
        self.partner = self.device(self.y, self.z, 1 - self.core)
        self.facing = self.device(1 - self.y, self.z, self.core)
        self.mate_z = self.z + 1 - 2 * lax.rem(self.z, 2)
        self.mate, self.far = self.device(self.y, self.mate_z, self.core), self.device(self.y, 3 - self.z, self.core)

    @staticmethod
    def device(y, z, core):
        return (y * ROW + z) * 2 + core

    def copy(self, name, src, dst, send, recv, device):
        out, into = self.sems[name]
        return remote(src, dst, out.at[send], into.at[recv], device)

    def keep40(self, c, part, gate, up):
        first = self.core == 0
        cols = pl.ds(pl.multiple_of(part * FB, FB), FB)
        for kind, g in enumerate((gate, up)):
            g = g.reshape(CHIPS, 2, -1, FB)
            self.own40[c, :, kind, :, cols] = jnp.where(first, g[:, 0], g[:, 1]).astype(BF16)
            self.stage40[lax.rem(c, 2), :, kind, :, cols] = jnp.where(first, g[:, 1], g[:, 0]).astype(BF16)

    def keep64(self, c, part, down):
        first = self.core == 0
        g = down.reshape(2, *self.own64.shape[2:])
        self.own64[c, part] = jnp.where(first, g[0], g[1]).astype(BF16)
        self.stage64[lax.rem(c, 2), part] = jnp.where(first, g[1], g[0]).astype(BF16)

    def pair40(self, c):
        return self.copy("pair40", self.stage40.at[lax.rem(c, 2)], self.peer40.at[c], c, c, self.partner)

    def pair64(self, c):
        return self.copy("pair64", self.stage64.at[lax.rem(c, 2)], self.peer64.at[c], c, c, self.partner)

    def y40(self, c):
        return self.copy("y40", self.own40.at[c, pl.ds((1 - self.y) * ROW, 4)], self.across40.at[c], c, c, self.facing)

    def y64(self, c):
        return self.copy("y64", self.own64.at[c, 1 - self.y], self.across64.at[c], c, c, self.facing)

    def z40(self, c, i):
        to = (self.mate_z, 3 - self.mate_z)[i]
        return self.copy("z40", self.own40.at[c, self.y * ROW + to], self.along40.at[c, i], (c, i), (c, i), self.mate)

    def far40(self, c):
        return self.copy("far40", self.own40.at[c, self.y * ROW + 3 - self.z], self.along40.at[c, 2], c, c, self.far)

    def z64(self, c, i):
        return self.copy("z64", self.own64.at[c, self.y], self.along64.at[i], (0, i), (0, i), self.mate)

    def far64(self, c):
        return self.copy("far64", self.own64.at[c, self.y], self.along64.at[2], 0, 0, self.far)

    def first_copy(self, c, i):
        at = (LAST, i)
        return self.copy("z64", self.own64.at[c], self.both64.at[i], at, at, self.mate)

    def second_copy(self, c):
        return self.copy("far64", self.own64.at[c], self.both64.at[2], LAST, LAST, self.far)

    def pair_sum(self, c, row):
        return wide(self.own64.at[c, row]) + wide(self.peer64.at[c, row])

    def row_sum(self, c, row):
        return self.pair_sum(c, row) + wide(self.both64.at[0, row]) + wide(self.both64.at[2, row])

    def first64(self, c):
        self.pair64(c).wait_recv()
        for i, owner in enumerate((self.mate_z, 3 - self.mate_z)):

            @pl.when(owner == lax.rem(c, ROW))
            def _():
                for row in range(2):
                    self.own64[c, row] = self.pair_sum(c, row).astype(BF16)
                self.first_copy(c, i).start()

    def second64(self, c):
        @pl.when(3 - self.z == lax.rem(c, ROW))
        def _():
            self.first_copy(c, 1).wait_recv()
            for row in range(2):
                self.own64[c, row] = (self.pair_sum(c, row) + wide(self.both64.at[1, row])).astype(BF16)
            self.second_copy(c).start()

    def third64(self):
        c = ROW + self.z
        self.first_copy(c, 0).wait_recv()
        self.second_copy(c).wait_recv()
        self.own64[c, 1 - self.y] = self.row_sum(c, 1 - self.y).astype(BF16)
        self.y64(c).start()

    def last64(self, g64):
        c = ROW + self.z
        self.y64(c).wait_recv()
        total = (self.row_sum(c, self.y) + wide(self.across64.at[c])).astype(BF16)
        g64[0] = total
        total = total.astype(F32)
        self.sq64[...] += total * total

    def over40(self, c):
        self.pair40(c).wait_recv()

        @pl.loop(0, ROW)
        def _(z):
            q = (1 - self.y) * ROW + z
            mine = self.own40.at[c, q]
            mine[...] = (wide(mine) + wide(self.peer40.at[c, q])).astype(BF16)

        self.y40(c).start()

    def over64(self, c):
        self.pair64(c).wait_recv()
        mine = self.own64.at[c, 1 - self.y]
        mine[...] = (wide(mine) + wide(self.peer64.at[c, 1 - self.y])).astype(BF16)
        self.y64(c).start()

    def sum40(self, c, z):
        q = self.y * ROW + z
        return wide(self.own40.at[c, q]) + wide(self.peer40.at[c, q]) + wide(self.across40.at[c, z])

    def sum64(self, c):
        return wide(self.own64.at[c, self.y]) + wide(self.peer64.at[c, self.y]) + wide(self.across64.at[c])

    def on40(self, c):
        self.y40(c).wait_recv()
        for i, to in enumerate((self.mate_z, 3 - self.mate_z)):
            self.own40[c, self.y * ROW + to] = self.sum40(c, to).astype(BF16)
            self.z40(c, i).start()

    def on64(self, c):
        self.y64(c).wait_recv()
        for i, owner in enumerate((self.mate_z, 3 - self.mate_z)):

            @pl.when(owner == lax.rem(c, ROW))
            def _():
                self.own64[c, self.y] = self.sum64(c).astype(BF16)
                self.z64(c, i).start()

    def out40(self, c):
        self.z40(c, 1).wait_recv()
        to = 3 - self.z
        self.own40[c, self.y * ROW + to] = (self.sum40(c, to) + wide(self.along40.at[c, 1])).astype(BF16)
        self.far40(c).start()

    def out64(self, c):
        @pl.when(3 - self.z == lax.rem(c, ROW))
        def _():
            self.z64(c, 1).wait_recv()
            self.own64[c, self.y] = (self.sum64(c) + wide(self.along64.at[1])).astype(BF16)
            self.far64(c).start()

    def end40(self, c, g40):
        self.z40(c, 0).wait_recv()
        self.far40(c).wait_recv()
        total = (self.sum40(c, self.z) + wide(self.along40.at[c, 0]) + wide(self.along40.at[c, 2])).astype(BF16)
        for part in range(2):
            cols = pl.ds(pl.multiple_of((lax.rem(c, ROW) + 4 * part) * FB, FB), FB)
            g40[:, 1 - lax.div(c, ROW), :, cols] = total[:, :, part * FB : (part + 1) * FB]
        total = total.astype(F32)
        self.sq40[...] += total * total

    def end64(self, c, g64):
        @pl.when(self.z == lax.rem(c, ROW))
        def _():
            self.z64(c, 0).wait_recv()
            self.far64(c).wait_recv()
            total = (self.sum64(c) + wide(self.along64.at[0]) + wide(self.along64.at[2])).astype(BF16)
            g64[1] = total
            total = total.astype(F32)
            self.sq64[...] += total * total

    def drain(self):
        for c in (6, 7):
            self.pair40(c).wait_send()
            self.pair64(c).wait_send()

        @pl.loop(0, 8)
        def _(c):
            self.far40(c).wait_send()
            self.y40(c).wait_send()
            for i in range(2):
                self.z40(c, i).wait_send()

        @pl.loop(0, ROW)
        def _(c):
            self.y64(c).wait_send()

        self.y64(ROW + self.z).wait_send()
        self.far64(0).wait_send()
        self.second_copy(4).wait_send()
        for i in range(2):
            self.z64(0, i).wait_send()
            self.first_copy(4, i).wait_send()


def backward_kernel(dy_in, a_in, h_in, dyt_in, a0t_in, wg, wu, wd, silu, slope, inner0, g40, g64, squares, *refs):
    d, a, dt, at, da, inner, dg, du, sems = refs[:9]
    stream = Stream(refs[9:])
    step = pl.program_id(0)
    half = pl.num_programs(0) // 3
    tokens = d.shape[0]

    def load(src, dst, i):
        return pltpu.make_async_copy(src, dst, sems.at[i])

    part, block = lax.rem(step, 2), lax.rem(lax.div(step, 2), 4)

    def gate_up(c):
        @pl.when((part == 0) & (c >= 2))
        def _():
            stream.pair40(c - 2).wait_send()

        stream.keep40(c, part, nn(at[...], dg[...]), nn(at[...], du[...]))

        @pl.when(part == 1)
        def _():
            stream.pair40(c).start()

    def down(c, inner):
        @pl.when((part == 0) & (c >= 2))
        def _():
            stream.pair64(c - 2).wait_send()

        stream.keep64(c, part, nn(dt[...], inner[...]).T)

        @pl.when(part == 1)
        def _():
            stream.pair64(c).start()

    @pl.when(step == 0)
    def _():
        for device in (stream.mate, stream.far, stream.partner, stream.facing):
            pl.semaphore_signal(pltpu.get_barrier_semaphore(), inc=1, device_id={"dp": device}, device_id_type=MESH)
        first = [load(dy_in, d, 0), load(a_in, a, 1), load(dyt_in, dt, 2)]
        for c in first:
            c.start()
        for r in tiles(tokens):
            da[r] = jnp.zeros((TILE, d.shape[1]), F32)
        stream.sq40[...] = jnp.zeros_like(stream.sq40)
        stream.sq64[...] = jnp.zeros_like(stream.sq64)
        for c in first:
            c.wait()
        at[...] = a[...].T

    @pl.when(step == 1)
    def _():
        pl.semaphore_wait(pltpu.get_barrier_semaphore(), 4)

    @pl.when(step < half)
    def _():
        both = jnp.concatenate([wg[...], wu[...]], axis=1)
        for r in tiles(tokens):
            by_inner = nt(d[r], wd[...]).astype(BF16).astype(F32)
            silu, slope, product = gates(a[r], wg[...], wu[...])
            by_gate, by_up = (by_inner * slope).astype(BF16), (by_inner * silu).astype(BF16)
            inner[r], dg[r], du[r] = product, by_gate, by_up
            da[r] += nt(jnp.concatenate([by_gate, by_up], axis=1), both)
        c = lax.div(step, 2) - 1

        @pl.when((part == 0) & (c >= 0))
        def _():
            stream.over64(c)
            stream.over40(c)

        @pl.when((part == 1) & (c >= 0))
        def _():
            stream.on64(c)
            stream.on40(c)

        @pl.when((part == 0) & (c >= 1))
        def _():
            stream.out64(c - 1)
            stream.out40(c - 1)

        @pl.when((part == 0) & (c >= 2))
        def _():
            stream.end64(c - 2, g64)
            stream.end40(c - 2, g40)

        @pl.when(step == half - 1)
        def _():
            load(h_in, a, 1).start()

        down(block, inner)
        gate_up(block)

    @pl.when(step == half - 1)
    def _():
        c = load(a0t_in, at, 0)
        c.start()
        load(h_in, a, 1).wait()
        for r in tiles(tokens):
            h = a[r].astype(F32)
            scale = lax.rsqrt(jnp.mean(h**2, -1, keepdims=True) + 1e-6)
            by_a = da[r].astype(BF16).astype(F32)
            by_h = scale * by_a - h * (scale**3 * jnp.mean(by_a * h, -1, keepdims=True))
            d[r] = d[r] + by_h.astype(BF16)
        dt[...] = d[...].T
        c.wait()

    @pl.when((step >= half) & (step < 2 * half))
    def _():
        @pl.when(step == half)
        def _():
            stream.out64(2)
            stream.out40(2)

        @pl.when(step == half + 1)
        def _():
            stream.over64(3)
            stream.over40(3)

        @pl.when(step == half + 2)
        def _():
            stream.end64(1, g64)
            stream.end40(1, g40)

        @pl.when((part == 1) & (block >= 1))
        def _():
            stream.first64(3 + block)

        @pl.when(step == half + 5)
        def _():
            stream.on64(3)
            stream.on40(3)

        down(ROW + block, inner0)

    @pl.when(step >= 2 * half)
    def _():
        for r in tiles(tokens):
            by_inner = nt(d[r], wd[...]).astype(BF16).astype(F32)
            dg[r], du[r] = (by_inner * slope[r]).astype(BF16), (by_inner * silu[r]).astype(BF16)

        @pl.when(step == 2 * half)
        def _():
            stream.first64(7)
            stream.end64(2, g64)
            stream.end40(2, g40)

        @pl.when((block >= 1) & (part == 0))
        def _():
            stream.over40(3 + block)

        @pl.when(step == 2 * half + 1)
        def _():
            stream.out64(3)
            stream.out40(3)

        @pl.when((step > 2 * half + 2) & (step <= 2 * half + 6))
        def _():
            stream.second64(1 + step - 2 * half)

        @pl.when(step == 2 * half + 5)
        def _():
            stream.end64(3, g64)
            stream.end40(3, g40)

        @pl.when((block >= 2) & (part == 1))
        def _():
            stream.on40(2 + block)

        gate_up(ROW + block)

    @pl.when(step == 3 * half - 1)
    def _():
        stream.over40(7)
        stream.out40(4)
        stream.on40(6)

        stream.third64()
        stream.out40(5)
        stream.end40(4, g40)
        stream.on40(7)
        stream.out40(6)
        stream.out40(7)
        stream.end40(5, g40)
        stream.end40(6, g40)
        stream.last64(g64)
        stream.end40(7, g40)
        stream.drain()
        total = jnp.sum(jnp.sum(stream.sq40[...], axis=0), keepdims=True) + jnp.sum(stream.sq64[...], keepdims=True)
        squares[...] = jnp.broadcast_to(total, squares.shape)


def backward(dy, a1, h1, dyt, a0t, wg, wu, wd, silu, slope, inner0):
    tokens, d = dy.shape
    ff = wg.shape[2]
    half = ff // FB
    early = lambda s: jnp.minimum(s, half - 1)
    late = lambda s: jnp.maximum(s - 2 * half, 0)
    middle = lambda s: jnp.clip(s - half, 0, half - 1)
    turn = lambda s: s // 2 + half // 2 * (s % 2)
    wcols = pl.BlockSpec((None, d, FB), lambda s: (1, 0, turn(early(s))))
    wrows = pl.BlockSpec((None, FB, d), lambda s: (1 - jnp.minimum(s // half, 1), turn(jnp.where(s < half, s, late(s))), 0))
    saved = pl.BlockSpec((tokens, FB), lambda s: (0, turn(late(s))))
    product = pl.BlockSpec((tokens, FB), lambda s: (0, turn(middle(s))))
    rows, block = pltpu.VMEM((tokens, d), BF16), pltpu.VMEM((tokens, FB), BF16)
    flipped = pltpu.VMEM((d, tokens), BF16)
    dma = pltpu.SemaphoreType.DMA
    of40 = lambda *s: pltpu.VMEM((*s, 2, 40, 2 * FB), BF16)
    of64 = lambda *s: pltpu.VMEM((*s, 128, 640), BF16)
    comms = [of40(8, CHIPS), of40(8, CHIPS), of40(8, 4), of40(8, 3), of40(2, CHIPS)]
    comms += [of64(8, 2), of64(8, 2), of64(8), of64(3), of64(2, 2)]
    comms += [pltpu.VMEM((2, 40, 2 * FB), F32), pltpu.VMEM((128, 640), F32), of64(3, 2)]
    comms += [dma((8,))] * 8 + [dma((8, 2))] * 2 + [dma((2, 2))] * 2 + [dma((8,))] * 2 + [dma((2,))] * 2
    return pl.pallas_call(
        backward_kernel,
        grid=(3 * half,),
        in_specs=[ANY] * 5 + [wcols, wcols, wrows, saved, saved, product],
        out_specs=[pl.BlockSpec(memory_space=pltpu.VMEM)] * 3,
        out_shape=[pltpu.VMEM((2, 2, 40, ff), BF16), pltpu.VMEM((2, 128, 640), BF16), pltpu.VMEM((8, 128), F32)],
        scratch_shapes=[rows, rows, flipped, flipped, pltpu.VMEM((tokens, d), F32), block, block, block, dma((3,))] + comms,
        compiler_params=pltpu.CompilerParams(collective_id=1, has_side_effects=True, vmem_limit_bytes=62 * MIB),
        name="backward",
    )(dy, a1, h1, dyt, a0t, wg, wu, wd, silu, slope, inner0)


def comm_kernel(n, count, *refs):
    it = iter(refs)
    take = lambda k: [next(it) for _ in range(k)]
    g40, g64, own_squares = take(3)
    ws, ms, vs = take(3), take(3), take(3)
    w_out, m_out, v_out = take(3), take(3), take(3)
    w40, w64, m40, m64, v40, v64, squares, local_sem = take(8)
    sq_send, sq_recv, gat_send, gat_recv, cross_send, cross_recv = take(6)

    here = Place()
    me, core = here.me, here.core
    streams = [(layer, kind) for kind in range(4) for layer in (1, 0)]
    sign = lambda kind: 1 - 2 * (kind % 2)
    loads = []

    def load(src, dst):
        c = pltpu.make_async_copy(src, dst, local_sem.at[len(loads)])
        c.start()
        loads.append(c)

    for side, x40, x64, per in ((ws, w40, w64, True), (ms, m40, m64, False), (vs, v40, v64, False)):
        for i in range(2):
            load(side[i].at[:, me] if per else side[i], x40.at[i])
        load(side[2].at[:, me] if per else side[2], x64)

    greet(n)
    squares[me] = own_squares[...]

    def tell(j):
        return remote(squares.at[me], squares.at[me], sq_send.at[j], sq_recv.at[me], lax.rem(me + j, n))

    def told(j):
        o = lax.rem(me + n - j, n)
        return remote(squares.at[o], squares.at[o], sq_send.at[j], sq_recv.at[o], o)

    @pl.loop(1, n)
    def _(j):
        tell(j).start()

    for c in loads:
        c.wait()

    @pl.loop(1, n)
    def _(j):
        told(j).wait_recv()

    total = jnp.sum(squares[...], axis=0)[:1, :1]
    factor = jnp.minimum(1.0, 0.5 * lax.rsqrt(total / count + 1e-30))

    def whole(layer, kind, owner):
        return w_out[kind].at[layer, owner] if kind < 2 else w_out[2].at[layer, owner, kind - 2]

    def pass_on(i, layer, kind, t):
        o = here.device_at(-sign(kind) * t)
        block = whole(layer, kind, o)
        return remote(block, block, gat_send.at[i, t], gat_recv.at[i, t], here.device_at(sign(kind)))

    def across(i, layer, kind, t):
        o = here.device_at(-sign(kind) * t)
        block = whole(layer, kind, o)
        return remote(block, block, cross_send.at[i, t], cross_recv.at[i, t], here.partner)

    def across_in(i, layer, kind, t):
        o = here.chip_at(-sign(kind) * t) * 2 + 1 - core
        block = whole(layer, kind, o)
        return remote(block, block, cross_send.at[i, t], cross_recv.at[i, t], here.partner)

    for i, (layer, kind) in enumerate(streams):
        sel = (lambda r40, r64: r40.at[kind, layer] if kind < 2 else r64.at[layer, kind - 2])
        out = (lambda r: r[kind].at[layer] if kind < 2 else r[2].at[layer, kind - 2])
        g = wide(g40.at[kind, layer] if kind < 2 else g64.at[layer, pl.ds((kind - 2) * 64, 64)]) * factor
        w, m, v = adamw(wide(sel(w40, w64)), sel(m40, m64)[...], sel(v40, v64)[...], g)
        whole(layer, kind, me)[...] = w
        pass_on(i, layer, kind, 0).start()
        across(i, layer, kind, 0).start()
        out(m_out)[...] = m
        out(v_out)[...] = v

    @pl.loop(1, HOPS)
    def _(t):
        for i, (layer, kind) in enumerate(streams):
            pass_on(i, layer, kind, t - 1).wait_recv()
            pass_on(i, layer, kind, t).start()
            across(i, layer, kind, t).start()

    for i, (layer, kind) in enumerate(streams):
        pass_on(i, layer, kind, HOPS - 1).wait_recv()
        across(i, layer, kind, HOPS).start()

    @pl.loop(0, HOPS)
    def _(t):
        for i, (layer, kind) in enumerate(streams):
            pass_on(i, layer, kind, t).wait_send()

    @pl.loop(1, n)
    def _(j):
        tell(j).wait_send()

    @pl.loop(0, CHIPS)
    def _(t):
        for i, (layer, kind) in enumerate(streams):
            across(i, layer, kind, t).wait_send()
            across_in(i, layer, kind, t).wait_recv()


def comm(n, count, grads, ws, ms, vs):
    dma = pltpu.SemaphoreType.DMA
    scratch = [pltpu.VMEM((2, 2, 40, 2048), BF16), pltpu.VMEM((2, 2, 64, 640), BF16)]
    scratch += [pltpu.VMEM((2, 2, 40, 2048), F32), pltpu.VMEM((2, 2, 64, 640), F32)] * 2
    scratch += [pltpu.VMEM((n, 8, 128), F32), dma((9,)), dma((n,)), dma((n,))]
    scratch += [dma((8, HOPS)), dma((8, HOPS)), dma((8, CHIPS)), dma((8, CHIPS))]
    out_shape = [pltpu.VMEM((2, n, 40, 2048), BF16)] * 2 + [pltpu.VMEM((2, n, 2, 64, 640), BF16)]
    out_shape += [pltpu.VMEM(a.shape, F32) for a in (*ms, *vs)]
    return pl.pallas_call(
        lambda *refs: comm_kernel(n, count, *refs),
        out_shape=out_shape,
        in_specs=[pl.BlockSpec(memory_space=pltpu.VMEM)] * 3 + [ANY] * 9,
        out_specs=[pl.BlockSpec(memory_space=pltpu.VMEM)] * 9,
        scratch_shapes=scratch,
        compiler_params=pltpu.CompilerParams(collective_id=0, has_side_effects=True, vmem_limit_bytes=40 * MIB),
        name="comm",
    )(*grads, *ws, *ms, *vs)


def write_kernel(*refs):
    k = (len(refs) - 1) // 2
    copies = [pltpu.make_async_copy(refs[i], refs[k + i], refs[-1].at[i]) for i in range(k)]
    for c in copies:
        c.start()
    for c in copies:
        c.wait()


def write(arrays):
    return pl.pallas_call(
        write_kernel,
        out_shape=[jax.ShapeDtypeStruct(a.shape, a.dtype) for a in arrays],
        in_specs=[pl.BlockSpec(memory_space=pltpu.VMEM)] * len(arrays),
        out_specs=[ANY] * len(arrays),
        scratch_shapes=[pltpu.SemaphoreType.DMA((len(arrays),))],
        compiler_params=pltpu.CompilerParams(vmem_limit_bytes=MIB),
        name="write",
    )(*arrays)


def solution(mesh):
    n = mesh.shape["dp"]

    def body(x, dy, wg, wu, wd, mg, mu, md, vg, vu, vd):
        x, dy = x[0], dy[0]
        silu, slope, inner0, a0t, dyt, h1, a1 = forward(x, dy, wg, wu, wd)
        grads = backward(dy, a1, h1, dyt, a0t, wg, wu, wd, silu, slope, inner0)
        rows = lambda w: w.reshape(w.shape[0], n, -1, w.shape[2])
        ws = [rows(wg), rows(wu), wd.reshape(2, n, 2, 64, 640)]
        split = lambda t: t.reshape(2, 2, 64, 640)
        count = wg.size + wu.size + wd.size
        outs = write(comm(n, count, grads, ws, [mg, mu, split(md)], [vg, vu, split(vd)]))
        shapes = [wg, wu, wd, mg, mu, md, vg, vu, vd]
        return tuple(o.reshape(s.shape) for o, s in zip(outs, shapes, strict=True))

    whole, mine = P(), P(None, "dp", None)
    seq, out = P(("rep", "dp")), P("rep", "dp", None)
    return jax.shard_map(
        body,
        mesh=mesh,
        in_specs=(seq, seq) + (whole,) * 3 + (mine,) * 6,
        out_specs=(P("rep"),) * 3 + (out,) * 6,
        check_vma=False,
    )
```
